32 devices in a mesh: dp: 2 (over x), tp: 4 (over z), sp: 4 (over y, core).
Axes of the slice: x: 2, y: 2, z: 4, core: 2. Of those that a mesh axis runs over, the one named last changes fastest.
Arguments:
- layer_in: bfloat16 [128, 5120], P('dp'), parts along dimension 0
- new_pos: int32 [128], P('dp'), parts along dimension 0
- k_cache: bfloat16 [128, 512, 8, 128], P('dp', 'sp', 'tp'), parts along dimension 0
- v_cache: bfloat16 [128, 512, 8, 128], P('dp', 'sp', 'tp'), parts along dimension 0
- attn_gain: bfloat16 [5120], replicated
- w_query: bfloat16 [5120, 4096], P(None, 'tp')
- w_key: bfloat16 [5120, 1024], P(None, 'tp')
- w_value: bfloat16 [5120, 1024], P(None, 'tp')
- w_out: bfloat16 [4096, 5120], P('tp')
- mlp_gain: bfloat16 [5120], replicated
- w_gate: bfloat16 [5120, 14336], P(None, 'tp')
- w_up: bfloat16 [5120, 14336], P(None, 'tp')
- w_down: bfloat16 [14336, 5120], P('tp')
Outputs:
- output 1: bfloat16 [128, 5120], P('dp'), parts along dimension 0
- output 2: bfloat16 [128, 512, 8, 128], P('dp', 'sp', 'tp'), parts along dimension 0
- output 3: bfloat16 [128, 512, 8, 128], P('dp', 'sp', 'tp'), parts along dimension 0
- output 4: bfloat16 [128, 8, 128], P('dp', 'tp'), parts along dimension 0
- output 5: bfloat16 [128, 8, 128], P('dp', 'tp'), parts along dimension 0
There are 2 independent parts. The reference program is written for one: setup_inputs(seed, part) draws one part's arguments, and reference() takes and returns one part's arrays. A program takes and returns all parts, laid end to end along the dimension named above; an argument that names none is the same for every part.
All inputs are finite; a program needn't handle non-finite values.
Results may differ from the reference program's by a relative error of at most 0.0049299.
Values sent between devices are 32-bit elements.
A program may use at most 1 GiB of HBM per device.

```python
import jax
import jax.numpy as jnp
from jax import lax

BATCH_ROWS = 64
CACHE_LEN = 512
MODEL_DIM = 5120
NUM_HEADS = 32
KV_HEADS = 8
HEAD_DIM = 128
FFN_DIM = 14336
ROPE_THETA = 1000000
COARSE_GROUPS = 64
GROUP_SIZE = NUM_HEADS // KV_HEADS
SCORE_SCALE = HEAD_DIM ** -0.5
MIN_POS = CACHE_LEN // 16


def weight(key_w, w_shape, fan_in):
    return (jax.random.normal(key_w, w_shape, jnp.float32) * fan_in ** -0.5).astype(jnp.bfloat16)


def setup_inputs(seed: int = 0, part: int = 0) -> dict:
    part_key = jax.random.fold_in(jax.random.key(seed), part)
    row_keys = jax.random.split(part_key, 7)
    w_keys = jax.random.split(jax.random.key(seed + 1), 9)
    layer_in = jax.random.normal(row_keys[0], (BATCH_ROWS, MODEL_DIM), jnp.float32).astype(jnp.bfloat16)
    pos_draw = jax.random.randint(row_keys[1], (BATCH_ROWS,), MIN_POS, CACHE_LEN)
    new_pos = jnp.where(jnp.arange(BATCH_ROWS) == 0, CACHE_LEN - 1, pos_draw).astype(jnp.int32)
    cache_shape = (BATCH_ROWS, CACHE_LEN, KV_HEADS, HEAD_DIM)
    coarse_shape = (BATCH_ROWS, COARSE_GROUPS, 1, KV_HEADS, HEAD_DIM)
    span_shape = (BATCH_ROWS, COARSE_GROUPS, CACHE_LEN // COARSE_GROUPS, KV_HEADS, HEAD_DIM)
    k_coarse = jnp.broadcast_to(jax.random.normal(row_keys[2], coarse_shape, jnp.float32), span_shape).reshape(cache_shape)
    v_coarse = jnp.broadcast_to(jax.random.normal(row_keys[3], coarse_shape, jnp.float32), span_shape).reshape(cache_shape)
    k_cache = (jax.random.normal(row_keys[4], cache_shape, jnp.float32) + 1.5 * k_coarse).astype(jnp.bfloat16)
    v_cache = (0.5 * jax.random.normal(row_keys[5], cache_shape, jnp.float32) + 2.0 * v_coarse).astype(jnp.bfloat16)
    attn_gain = (1.0 + 0.2 * jax.random.normal(w_keys[0], (MODEL_DIM,), jnp.float32)).astype(jnp.bfloat16)
    mlp_gain = (1.0 + 0.2 * jax.random.normal(w_keys[1], (MODEL_DIM,), jnp.float32)).astype(jnp.bfloat16)
    return {
        'layer_in': layer_in,
        'new_pos': new_pos,
        'k_cache': k_cache,
        'v_cache': v_cache,
        'attn_gain': attn_gain,
        'w_query': weight(w_keys[2], (MODEL_DIM, NUM_HEADS * HEAD_DIM), MODEL_DIM),
        'w_key': weight(w_keys[3], (MODEL_DIM, KV_HEADS * HEAD_DIM), MODEL_DIM),
        'w_value': weight(w_keys[4], (MODEL_DIM, KV_HEADS * HEAD_DIM), MODEL_DIM),
        'w_out': weight(w_keys[5], (NUM_HEADS * HEAD_DIM, MODEL_DIM), NUM_HEADS * HEAD_DIM),
        'mlp_gain': mlp_gain,
        'w_gate': weight(w_keys[6], (MODEL_DIM, FFN_DIM), MODEL_DIM),
        'w_up': weight(w_keys[7], (MODEL_DIM, FFN_DIM), MODEL_DIM),
        'w_down': weight(w_keys[8], (FFN_DIM, MODEL_DIM), FFN_DIM),
    }


def rms_norm(in_vec, gain_vec):
    mean_sq = jnp.mean(jnp.square(in_vec), axis=-1, keepdims=True)
    return in_vec * lax.rsqrt(mean_sq + 1e-5) * gain_vec.astype(jnp.float32)


def apply_rotary(in_vec, positions):
    half_idx = jnp.arange(HEAD_DIM // 2, dtype=jnp.float32)
    inv_freq = 1.0 / (ROPE_THETA ** (2.0 * half_idx / HEAD_DIM))
    angles = positions.astype(jnp.float32)[:, None] * inv_freq[None, :]
    cos_a = jnp.cos(angles)[:, None, :]
    sin_a = jnp.sin(angles)[:, None, :]
    pair_view = in_vec.reshape(in_vec.shape[:-1] + (HEAD_DIM // 2, 2))
    even_part = pair_view[..., 0]
    odd_part = pair_view[..., 1]
    rotated = jnp.stack([even_part * cos_a - odd_part * sin_a, even_part * sin_a + odd_part * cos_a], axis=-1)
    return rotated.reshape(in_vec.shape)


def reference(layer_in, new_pos, k_cache, v_cache, attn_gain, w_query, w_key, w_value, w_out, mlp_gain, w_gate, w_up, w_down):
    x_f32 = layer_in.astype(jnp.float32)
    normed = rms_norm(x_f32, attn_gain).astype(jnp.bfloat16)
    q_proj = jnp.dot(normed, w_query, preferred_element_type=jnp.float32).reshape(BATCH_ROWS, NUM_HEADS, HEAD_DIM)
    k_proj = jnp.dot(normed, w_key, preferred_element_type=jnp.float32).reshape(BATCH_ROWS, KV_HEADS, HEAD_DIM)
    v_new = jnp.dot(normed, w_value, preferred_element_type=jnp.float32).reshape(BATCH_ROWS, KV_HEADS, HEAD_DIM).astype(jnp.bfloat16)
    q_rot = apply_rotary(q_proj, new_pos).astype(jnp.bfloat16)
    k_rot = apply_rotary(k_proj, new_pos).astype(jnp.bfloat16)
    slot_ids = jnp.arange(CACHE_LEN)

    def one_row(row_args):
        q_row, k_row, v_row, k_rows, v_rows, pos_row = row_args
        is_new = (slot_ids == pos_row)[:, None, None]
        k_upd = jnp.where(is_new, k_row[None], k_rows)
        v_upd = jnp.where(is_new, v_row[None], v_rows)
        q_grp = q_row.reshape(KV_HEADS, GROUP_SIZE, HEAD_DIM).astype(jnp.float32)
        scores = jnp.einsum('kgd,skd->kgs', q_grp, k_upd.astype(jnp.float32)) * SCORE_SCALE
        scores = jnp.where(slot_ids <= pos_row, scores, -jnp.inf)
        row_max = jnp.max(scores, axis=-1, keepdims=True)
        prob_vals = jnp.exp(scores - row_max)
        denom_sum = jnp.sum(prob_vals, axis=-1)
        weighted = jnp.einsum('kgs,skd->kgd', prob_vals.astype(jnp.bfloat16).astype(jnp.float32), v_upd.astype(jnp.float32))
        attn_row = (weighted / denom_sum[..., None]).reshape(NUM_HEADS * HEAD_DIM)
        return attn_row, k_upd, v_upd

    attn_rows, k_out, v_out = lax.map(one_row, (q_rot, k_rot, v_new, k_cache, v_cache, new_pos))
    attn_vec = attn_rows.astype(jnp.bfloat16)
    hidden = x_f32 + jnp.dot(attn_vec, w_out, preferred_element_type=jnp.float32)
    normed_mlp = rms_norm(hidden, mlp_gain).astype(jnp.bfloat16)
    gate_pre = jnp.dot(normed_mlp, w_gate, preferred_element_type=jnp.float32)
    up_proj = jnp.dot(normed_mlp, w_up, preferred_element_type=jnp.float32)
    act_bf = (jax.nn.silu(gate_pre) * up_proj).astype(jnp.bfloat16)
    layer_out = (hidden + jnp.dot(act_bf, w_down, preferred_element_type=jnp.float32)).astype(jnp.bfloat16)
    return (layer_out, k_out, v_out, k_rot, v_new)
```

```python
import functools

import jax
import jax.numpy as jnp
import numpy as np
from jax import lax
from jax.experimental import pallas as pl
from jax.experimental.pallas import tpu as pltpu
from jax.sharding import PartitionSpec as P

ROPE_THETA = 1000000
MESH = pl.DeviceIdType.MESH
F32 = jnp.float32
BF16 = jnp.bfloat16
NEG = float(np.finfo(np.float32).min)
VMEM_LIMIT = 62 * 1024 * 1024
ANY = pl.BlockSpec(memory_space=pl.ANY)
VM = pl.BlockSpec(memory_space=pltpu.VMEM)

ROWS = 64
DIM = 5120
HD = 128
HEADS = 8
KV = 2
BLK = 128
QKV = (HEADS + 2 * KV) * HD
KSTEP = 512
KCH = DIM // KSTEP
BCH = 8
NB = ROWS // BCH


def attend_kernel(pos_hbm, x_hbm, gain_hbm, freq_hbm, wq, wk, wv, kc, vc,
                  ko, vo, kn_ref, vn_ref, part_ref,
                  pos_s, x_v, gain_v, freq_v, w_v, k_v, v_v, n_v, acc, pos_v, qs, ks, vs,
                  sem_m, sem_w, sem_k, sem_v, sem_ko, sem_vo):
    sp = lax.axis_index('sp')

    small = [pltpu.make_async_copy(pos_hbm, pos_s, sem_m.at[0]),
             pltpu.make_async_copy(x_hbm, x_v, sem_m.at[1]),
             pltpu.make_async_copy(gain_hbm, gain_v, sem_m.at[2]),
             pltpu.make_async_copy(freq_hbm, freq_v, sem_m.at[3])]
    for cp in small:
        cp.start()

    def w_copies(i):
        rows = pl.ds(pl.multiple_of(i * KSTEP, KSTEP), KSTEP)
        return (pltpu.make_async_copy(wq.at[rows], w_v.at[rows, pl.ds(0, 1024)], sem_w.at[i, 0]),
                pltpu.make_async_copy(wk.at[rows], w_v.at[rows, pl.ds(1024, 256)], sem_w.at[i, 1]),
                pltpu.make_async_copy(wv.at[rows], w_v.at[rows, pl.ds(1280, 256)], sem_w.at[i, 2]))

    def cache_copy(src, dst, sem, i):
        rows = pl.ds(pl.multiple_of(i * BCH, BCH), BCH)
        return pltpu.make_async_copy(src.at[rows], dst.at[rows], sem.at[i])

    for i in range(KCH):
        for cp in w_copies(i):
            cp.start()
    for i in range(NB):
        cache_copy(kc, k_v, sem_k, i).start()
        cache_copy(vc, v_v, sem_v, i).start()

    for cp in small:
        cp.wait()
    for r in range(0, ROWS, 16):
        x = x_v[r:r + 16, :].astype(F32)
        inv = lax.rsqrt(jnp.mean(x * x, axis=-1, keepdims=True) + 1e-5)
        n_v[r:r + 16, :] = (x * inv * gain_v[...].astype(F32)).astype(BF16)
    for b in range(ROWS):
        pos_v[b:b + 1, :] = jnp.full((1, HD), pos_s[b], jnp.int32)
    angles = pos_v[...].astype(F32) * freq_v[...]
    cos_a = jnp.cos(angles)
    sin_a = jnp.sin(angles)
    odd = lax.broadcasted_iota(jnp.int32, (ROWS, HD), 1) % 2 == 1
    sin_a = jnp.where(odd, sin_a, -sin_a)

    acc[...] = jnp.zeros_like(acc)

    def w_step(i, carry):
        for cp in w_copies(i):
            cp.wait()
        rows = pl.ds(pl.multiple_of(i * KSTEP, KSTEP), KSTEP)
        acc[...] += jnp.dot(n_v[:, rows], w_v[rows, :], preferred_element_type=F32)
        return carry

    lax.fori_loop(0, KCH, w_step, 0)

    def rotate(val):
        swapped = jnp.where(odd, pltpu.roll(val, 1, 1), pltpu.roll(val, HD - 1, 1))
        return (val * cos_a + swapped * sin_a).astype(BF16).astype(F32)

    for h in range(HEADS):
        qs[pl.ds(h, ROWS, stride=HEADS), :] = rotate(acc[:, h * HD:(h + 1) * HD])
    for h in range(KV):
        lo = (HEADS + h) * HD
        ks[pl.ds(h, ROWS, stride=KV), :] = rotate(acc[:, lo:lo + HD])
        lo = (HEADS + KV + h) * HD
        vs[pl.ds(h, ROWS, stride=KV), :] = acc[:, lo:lo + HD].astype(BF16).astype(F32)
    kn_ref[...] = ks[...].astype(BF16)
    vn_ref[...] = vs[...].astype(BF16)

    row16 = lax.broadcasted_iota(jnp.int32, (16, HD), 0)
    lane = lax.broadcasted_iota(jnp.int32, (HEADS, KV * BLK), 1)
    group = lax.broadcasted_iota(jnp.int32, (HEADS, KV * BLK), 0) // (HEADS // KV)
    same_head = (lane % KV) == group
    lane_slot = lane // KV
    stat_lane = lax.broadcasted_iota(jnp.int32, (HEADS, HD), 1)

    def put_new(cache_v, new, b, slot):
        inside = jnp.logical_and(slot >= 0, slot < BLK)
        tile = jnp.where(inside, slot // 8, 0)
        local = jnp.where(inside, slot - tile * 8, -1)
        at = pl.ds(pl.multiple_of(tile * 16, 16), 16)
        old = cache_v[b, at, :].astype(F32)
        both = jnp.where(row16 % 2 == 0, new[pl.ds(2 * b, 1), :], new[pl.ds(2 * b + 1, 1), :])
        cache_v[b, at, :] = jnp.where(row16 // 2 == local, both, old).astype(BF16)

    def chunk(i, stat):
        cache_copy(kc, k_v, sem_k, i).wait()
        cache_copy(vc, v_v, sem_v, i).wait()
        slots = [pos_s[i * BCH + u] - sp * BLK for u in range(BCH)]
        for u in range(BCH):
            put_new(k_v, ks, i * BCH + u, slots[u])
            put_new(v_v, vs, i * BCH + u, slots[u])
        cache_copy(k_v, ko, sem_ko, i).start()
        cache_copy(v_v, vo, sem_vo, i).start()
        raw = []
        for u in range(BCH):
            b = i * BCH + u
            q = qs[pl.ds(pl.multiple_of(b * HEADS, HEADS), HEADS), :].astype(BF16)
            raw.append(lax.dot_general(q, k_v[b], (((1,), (1,)), ((), ())), preferred_element_type=F32))
        for u in range(BCH):
            b = i * BCH + u
            valid = jnp.logical_and(same_head, lane_slot <= slots[u])
            score = jnp.where(valid, raw[u] * (HD ** -0.5), NEG)
            top = jnp.max(score, axis=-1, keepdims=True)
            prob = jnp.where(valid, jnp.exp(score - top), 0.0)
            total = jnp.sum(prob, axis=-1, keepdims=True)
            out = jnp.dot(prob.astype(BF16), v_v[b], preferred_element_type=F32)
            half = b // 32
            part_ref[half, pl.ds(pl.multiple_of((b - half * 32) * HEADS, HEADS), HEADS), :] = out
            stat = jnp.where(stat_lane == b, top, stat)
            stat = jnp.where(stat_lane == b + ROWS, total, stat)
        return stat

    stat = lax.fori_loop(0, NB, chunk, jnp.zeros((HEADS, HD), F32))
    part_ref[0, 256:264, :] = stat
    part_ref[1, 256:264, :] = pltpu.roll(stat, 96, 1)
    for i in range(NB):
        cache_copy(k_v, ko, sem_ko, i).wait()
        cache_copy(v_v, vo, sem_vo, i).wait()


def attend(new_pos, x, gain, freq, wq, wk, wv, kc, vc):
    cache = jax.ShapeDtypeStruct(kc.shape, BF16)
    new = jax.ShapeDtypeStruct((ROWS * KV, HD), BF16)
    return pl.pallas_call(
        attend_kernel,
        out_shape=(cache, cache, new, new, jax.ShapeDtypeStruct((2, 264, HD), F32)),
        in_specs=[ANY] * 9,
        out_specs=(ANY, ANY, VM, VM, VM),
        scratch_shapes=[
            pltpu.SMEM((ROWS,), jnp.int32),
            pltpu.VMEM((ROWS, DIM), BF16),
            pltpu.VMEM((1, DIM), F32),
            pltpu.VMEM((1, HD), F32),
            pltpu.VMEM((DIM, QKV), BF16),
            pltpu.VMEM(kc.shape, BF16),
            pltpu.VMEM(vc.shape, BF16),
            pltpu.VMEM((ROWS, DIM), BF16),
            pltpu.VMEM((ROWS, QKV), F32),
            pltpu.VMEM((ROWS, HD), jnp.int32),
            pltpu.VMEM((ROWS * HEADS, HD), F32),
            pltpu.VMEM((ROWS * KV, HD), F32),
            pltpu.VMEM((ROWS * KV, HD), F32),
            pltpu.SemaphoreType.DMA((4,)),
            pltpu.SemaphoreType.DMA((KCH, 3)),
            pltpu.SemaphoreType.DMA((NB,)),
            pltpu.SemaphoreType.DMA((NB,)),
            pltpu.SemaphoreType.DMA((NB,)),
            pltpu.SemaphoreType.DMA((NB,)),
        ],
        compiler_params=pltpu.CompilerParams(vmem_limit_bytes=VMEM_LIMIT),
        name="attend",
    )(new_pos, x, gain, freq, wq, wk, wv, kc, vc)


TP = 4
COLS = DIM // 4
HID = 896
HCH = HID // 128
RB = ROWS // TP
NC = 2
CW = COLS // NC


def mix_kernel(part_ref, x_hbm, gain_hbm, wo, wg, wu, wd, out_ref,
               xb_v, gain_v, wo_v, wgu_v, wd_v,
               pa, pb, pc, at_o, lhs_v, mm, rs_buf, hfull, n2, act, act_b, ofull,
               sem_l, sem_g, sem_d, cs, cr, rs_s, rs_r, az_s, az_r, ay_s, ay_r, ac_s, ac_r,
               my_s, my_r, mc_s, mc_r):
    dp = lax.axis_index('dp')
    z = lax.axis_index('tp')
    sp = lax.axis_index('sp')
    y = sp // 2
    c = sp % 2
    sp_y = (1 - y) * 2 + c
    sp_c = y * 2 + (1 - c)
    sp_yc = (1 - y) * 2 + (1 - c)
    dev_y = (dp, z, sp_y)
    dev_c = (dp, z, sp_c)
    dev_z = [None] + [(dp, lax.rem(z + d, TP), sp) for d in range(1, TP)]
    src_z = [z] + [lax.rem(z + TP - d, TP) for d in range(1, TP)]

    def col_at(s, j=0, width=COLS):
        return pl.ds(pl.multiple_of(s * COLS + j * width, 128), width)

    def row_at(zz):
        return pl.ds(pl.multiple_of(zz * RB, RB), RB)

    loads = [pltpu.make_async_copy(wo.at[:, col_at(sp)], wo_v, sem_l.at[0]),
             pltpu.make_async_copy(x_hbm.at[row_at(z), col_at(sp)], xb_v, sem_l.at[1]),
             pltpu.make_async_copy(gain_hbm, gain_v, sem_l.at[2])]
    for cp in loads:
        cp.start()

    def gu_copies(j):
        cols = pl.ds(pl.multiple_of(sp * HID + j * 128, 128), 128)
        return (pltpu.make_async_copy(wg.at[:, cols], wgu_v.at[j, :, pl.ds(0, 128)], sem_g.at[j, 0]),
                pltpu.make_async_copy(wu.at[:, cols], wgu_v.at[j, :, pl.ds(128, 128)], sem_g.at[j, 1]))

    for j in range(HCH):
        for cp in gu_copies(j):
            cp.start()
    order = [sp, sp_c, sp_y, sp_yc]
    d_copies = [pltpu.make_async_copy(wd.at[pl.ds(pl.multiple_of(s * HID, 128), HID), col_at(sp)],
                                      wd_v.at[i], sem_d.at[i]) for i, s in enumerate(order)]
    for cp in d_copies:
        cp.start()

    barrier = pltpu.get_barrier_semaphore()
    for dev in [dev_y, dev_c] + dev_z[1:]:
        pl.semaphore_signal(barrier, inc=1, device_id=dev, device_id_type=MESH)
    pl.semaphore_wait(barrier, 5)

    sends = []

    def push(src, dst, ssem, rsem, dev):
        cp = pltpu.make_async_remote_copy(src_ref=src, dst_ref=dst, send_sem=ssem, recv_sem=rsem,
                                          device_id=dev, device_id_type=MESH)
        cp.start()
        sends.append(cp)
        return cp

    lane = lax.broadcasted_iota(jnp.int32, (HEADS, HD), 1)

    def weights(s1, s2):
        top = jnp.maximum(s1, s2)
        a1 = jnp.exp(s1 - top)
        a2 = jnp.exp(s2 - top)
        total = a1 * pltpu.roll(s1, 64, 1) + a2 * pltpu.roll(s2, 64, 1)
        return top, a1, a2, total

    cp = push(part_ref.at[1 - c], pa, cs.at[0], cr.at[0], dev_c)
    cp.wait_recv()
    top, a1, a2, total = weights(part_ref[c, 256:264, :], pa[256:264, :])
    for i in range(32):
        r = slice(i * 8, i * 8 + 8)
        pb[r, :] = a1[:, i:i + 1] * part_ref[c, r, :] + a2[:, i:i + 1] * pa[r, :]
    pb[256:264, :] = jnp.where(lane < 64, top, pltpu.roll(total, 64, 1))
    cp = push(pb, pc, cs.at[1], cr.at[1], dev_y)
    cp.wait_recv()
    top, a1, a2, total = weights(pb[256:264, :], pc[256:264, :])
    a1 = a1 / total
    a2 = a2 / total
    half = pl.multiple_of(c * 256, 256)
    for i in range(32):
        r = slice(i * 8, i * 8 + 8)
        at_o[pl.ds(pl.multiple_of(half + i * 8, 8), 8), :] = a1[:, i:i + 1] * pb[r, :] + a2[:, i:i + 1] * pc[r, :]
    mine = at_o.at[pl.ds(half, 256)]
    cp = push(mine, mine, cs.at[2], cr.at[2], dev_c)
    cp.wait_recv()
    for h in range(HEADS):
        lhs_v[:, h * HD:(h + 1) * HD] = at_o[pl.ds(h, ROWS, stride=HEADS), :].astype(BF16)

    def scatter(stage, j):
        cols = pl.ds(j * CW, CW)
        for d in range(1, TP):
            zz = lax.rem(z + d, TP)
            push(mm.at[stage, row_at(zz), cols], rs_buf.at[stage, d - 1, :, cols],
                 rs_s.at[stage, j, d - 1], rs_r.at[stage, j, d - 1], dev_z[d])

    def gather(stage, base, full):
        def blk(s, d, j):
            return full.at[row_at(src_z[d]), col_at(s, 0, COLS) if False else pl.ds(
                pl.multiple_of(s * COLS + j * CW, 128), CW)]

        def wait_in(ref, sem):
            pltpu.make_async_copy(ref, ref, sem).wait()

        for j in range(NC):
            cols = slice(j * CW, (j + 1) * CW)
            val = base(cols) + mm[stage, row_at(z), cols]
            for d in range(1, TP):
                wait_in(rs_buf.at[stage, d - 1, :, pl.ds(j * CW, CW)], rs_r.at[stage, j, d - 1])
                val = val + rs_buf[stage, d - 1, :, cols]
            full[row_at(z), pl.ds(pl.multiple_of(sp * COLS + j * CW, 128), CW)] = val
            own = blk(sp, 0, j)
            for d in range(1, TP):
                push(own, own, az_s.at[stage, j, d - 1], az_r.at[stage, j, d - 1], dev_z[d])
            push(own, own, ay_s.at[stage, j, 0], ay_r.at[stage, j, 0], dev_y)
            push(own, own, ac_s.at[stage, j, 0], ac_r.at[stage, j, 0], dev_c)
        for j in range(NC):
            for d in (1, 3, 2):
                ref = blk(sp, d, j)
                wait_in(ref, az_r.at[stage, j, d - 1])
                push(ref, ref, ay_s.at[stage, j, d], ay_r.at[stage, j, d], dev_y)
                push(ref, ref, ac_s.at[stage, j, d], ac_r.at[stage, j, d], dev_c)
        for j in range(NC):
            for d in (0, 1, 3, 2):
                ref = blk(sp_y, d, j)
                wait_in(ref, ay_r.at[stage, j, d])
                push(ref, ref, ac_s.at[stage, j, TP + d], ac_r.at[stage, j, TP + d], dev_c)
        for j in range(NC):
            for d in range(TP):
                wait_in(blk(sp_c, d, j), ac_r.at[stage, j, d])
                wait_in(blk(sp_yc, d, j), ac_r.at[stage, j, TP + d])

    for cp in loads:
        cp.wait()
    for j in range(NC):
        cols = slice(j * CW, (j + 1) * CW)
        mm[0, :, cols] = jnp.dot(lhs_v[...], wo_v[:, cols], preferred_element_type=F32)
        scatter(0, j)
    gather(0, lambda cols: xb_v[:, cols].astype(F32), hfull)

    for r in range(0, ROWS, 16):
        h = hfull[r:r + 16, :]
        inv = lax.rsqrt(jnp.mean(h * h, axis=-1, keepdims=True) + 1e-5)
        n2[r:r + 16, :] = (h * inv * gain_v[...].astype(F32)).astype(BF16)

    def act_copies(j):
        own = act.at[sp, j]
        return (pltpu.make_async_remote_copy(src_ref=own, dst_ref=own, send_sem=my_s.at[j], recv_sem=my_r.at[j],
                                             device_id=dev_y, device_id_type=MESH),
                pltpu.make_async_remote_copy(src_ref=own, dst_ref=own, send_sem=mc_s.at[0, j], recv_sem=mc_r.at[0, j],
                                             device_id=dev_c, device_id_type=MESH))

    def fwd_copy(j):
        ref = act.at[sp_y, j]
        return pltpu.make_async_remote_copy(src_ref=ref, dst_ref=ref, send_sem=mc_s.at[1, j], recv_sem=mc_r.at[1, j],
                                            device_id=dev_c, device_id_type=MESH)

    def hidden_step(j, carry):
        for cp in gu_copies(j):
            cp.wait()
        gu = jnp.dot(n2[...], wgu_v[j], preferred_element_type=F32)
        gate = gu[:, :128]
        val = gate * jax.nn.sigmoid(gate) * gu[:, 128:]
        act[sp, j] = val.astype(BF16).astype(F32)
        for cp in act_copies(j):
            cp.start()
        return carry

    lax.fori_loop(0, HCH, hidden_step, 0)

    def down(i, s):
        for j in range(HCH):
            act_b[:, j * 128:(j + 1) * 128] = act[s, j].astype(BF16)
        d_copies[i].wait()
        for k in range(0, COLS, 256):
            prod = jnp.dot(act_b[...], wd_v[i, :, k:k + 256], preferred_element_type=F32)
            if i == 0:
                mm[1, :, k:k + 256] = prod
            else:
                mm[1, :, k:k + 256] += prod

    down(0, sp)
    for j in range(HCH):
        act_copies(j)[1].wait_recv()
    down(1, sp_c)
    for j in range(HCH):
        act_copies(j)[0].wait_recv()
        fwd_copy(j).start()
    down(2, sp_y)
    for j in range(HCH):
        fwd_copy(j).wait_recv()
    down(3, sp_yc)
    for j in range(NC):
        scatter(1, j)

    own_h = hfull.at[row_at(z), col_at(sp)]
    gather(1, lambda cols: own_h[:, cols], ofull)
    out_ref[...] = ofull[...].astype(BF16)

    for cp in sends:
        cp.wait_send()
    for j in range(HCH):
        for cp in act_copies(j):
            cp.wait_send()
        fwd_copy(j).wait_send()


def mix(part, x, gain, wo, wg, wu, wd):
    dma = pltpu.SemaphoreType.DMA
    return pl.pallas_call(
        mix_kernel,
        out_shape=jax.ShapeDtypeStruct((ROWS, DIM), BF16),
        in_specs=[VM] + [ANY] * 6,
        out_specs=VM,
        scratch_shapes=[
            pltpu.VMEM((RB, COLS), BF16),
            pltpu.VMEM((1, DIM), F32),
            pltpu.VMEM((1024, COLS), BF16),
            pltpu.VMEM((HCH, DIM, 256), BF16),
            pltpu.VMEM((4, HID, COLS), BF16),
            pltpu.VMEM((264, HD), F32),
            pltpu.VMEM((264, HD), F32),
            pltpu.VMEM((264, HD), F32),
            pltpu.VMEM((ROWS * HEADS, HD), F32),
            pltpu.VMEM((ROWS, 1024), BF16),
            pltpu.VMEM((2, ROWS, COLS), F32),
            pltpu.VMEM((2, TP - 1, RB, COLS), F32),
            pltpu.VMEM((ROWS, DIM), F32),
            pltpu.VMEM((ROWS, DIM), BF16),
            pltpu.VMEM((4, HCH, ROWS, 128), F32),
            pltpu.VMEM((ROWS, HID), BF16),
            pltpu.VMEM((ROWS, DIM), F32),
            dma((3,)), dma((HCH, 2)), dma((4,)),
            dma((3,)), dma((3,)),
            dma((2, NC, 3)), dma((2, NC, 3)),
            dma((2, NC, 3)), dma((2, NC, 3)),
            dma((2, NC, TP)), dma((2, NC, TP)),
            dma((2, NC, 2 * TP)), dma((2, NC, 2 * TP)),
            dma((HCH,)), dma((HCH,)),
            dma((2, HCH)), dma((2, HCH)),
        ],
        compiler_params=pltpu.CompilerParams(vmem_limit_bytes=VMEM_LIMIT, collective_id=0, has_side_effects=True),
        name="mix",
    )(part, x, gain, wo, wg, wu, wd)


def solution(mesh):
    def local_step(layer_in, new_pos, k_blk, v_blk, attn_gain, w_query, w_key, w_value, w_out, mlp_gain, w_gate, w_up, w_down):
        half_idx = np.arange(HD // 2, dtype=np.float32)
        inv_freq = (1.0 / (np.float32(ROPE_THETA) ** (np.float32(2.0) * half_idx / np.float32(HD)))).astype(np.float32)
        freq = jnp.asarray(np.repeat(inv_freq, 2)[None, :])
        flat = (ROWS, BLK * KV, HD)
        k_out, v_out, k_new, v_new, part = attend(
            new_pos, layer_in, attn_gain.astype(F32).reshape(1, DIM), freq, w_query, w_key, w_value,
            k_blk.reshape(flat), v_blk.reshape(flat))
        layer_out = mix(part, layer_in, mlp_gain.astype(F32).reshape(1, DIM), w_out, w_gate, w_up, w_down)
        return (layer_out, k_out.reshape(k_blk.shape), v_out.reshape(v_blk.shape),
                k_new.reshape(ROWS, KV, HD), v_new.reshape(ROWS, KV, HD))

    cache_spec = P('dp', 'sp', 'tp', None)
    new_spec = P('dp', 'tp', None)
    in_specs = (P('dp', None), P('dp'), cache_spec, cache_spec, P(None), P(None, 'tp'), P(None, 'tp'), P(None, 'tp'), P('tp', None), P(None), P(None, 'tp'), P(None, 'tp'), P('tp', None))
    out_specs = (P('dp', None), cache_spec, cache_spec, new_spec, new_spec)
    return jax.shard_map(local_step, mesh=mesh, in_specs=in_specs, out_specs=out_specs, check_vma=False)
```

```python
import functools

import jax
import jax.numpy as jnp
import numpy as np
from jax import lax
from jax.experimental import pallas as pl
from jax.experimental.pallas import tpu as pltpu
from jax.sharding import PartitionSpec as P

ROPE_THETA = 1000000
MESH = pl.DeviceIdType.MESH
F32 = jnp.float32
BF16 = jnp.bfloat16
NEG = float(np.finfo(np.float32).min)
ATTEND_VMEM = 62 * 1024 * 1024
MIX_VMEM = 48 * 1024 * 1024
ANY = pl.BlockSpec(memory_space=pltpu.HBM)
VM = pl.BlockSpec(memory_space=pltpu.VMEM)

ROWS = 64
DIM = 5120
HD = 128
HEADS = 8
KV = 2
BLK = 128
QKV = (HEADS + 2 * KV) * HD
KSTEP = 1024
KCH = DIM // KSTEP
BCH = 8
NB = ROWS // BCH
LATE = 4


def attend_kernel(pos_hbm, x_hbm, gain_hbm, freq_hbm, wq, wk, wv, kc, vc,
                  ko, vo, kn_ref, vn_ref, part_ref,
                  pos_s, x_v, gain_v, freq_v, w_v, k_v, v_v, n_v, acc, pos_v, qs, ks, vs,
                  sem_m, sem_w, sem_k, sem_v, sem_ko, sem_vo):
    sp = lax.axis_index('sp')

    small = [pltpu.make_async_copy(pos_hbm, pos_s, sem_m.at[0]),
             pltpu.make_async_copy(x_hbm, x_v, sem_m.at[1]),
             pltpu.make_async_copy(gain_hbm, gain_v, sem_m.at[2]),
             pltpu.make_async_copy(freq_hbm, freq_v, sem_m.at[3])]
    for cp in small:
        cp.start()

    def w_copies(i):
        rows = pl.ds(pl.multiple_of(i * KSTEP, KSTEP), KSTEP)
        return (pltpu.make_async_copy(wq.at[rows], w_v.at[rows, pl.ds(0, 1024)], sem_w.at[i, 0]),
                pltpu.make_async_copy(wk.at[rows], w_v.at[rows, pl.ds(1024, 256)], sem_w.at[i, 1]),
                pltpu.make_async_copy(wv.at[rows], w_v.at[rows, pl.ds(1280, 256)], sem_w.at[i, 2]))

    def cache_copy(src, dst, sem, i):
        rows = pl.ds(pl.multiple_of(i * BCH, BCH), BCH)
        return pltpu.make_async_copy(src.at[rows], dst.at[rows], sem.at[i])

    for i in range(KCH):
        for cp in w_copies(i):
            cp.start()
    for cp in small:
        cp.wait()
    for r in range(0, ROWS, 16):
        x = x_v[r:r + 16, :].astype(F32)
        inv = lax.rsqrt(jnp.mean(x * x, axis=-1, keepdims=True) + 1e-5)
        n_v[r:r + 16, :] = (x * inv * gain_v[...].astype(F32).reshape(1, DIM)).astype(BF16)
    for b in range(ROWS):
        pos_v[b:b + 1, :] = jnp.full((1, HD), pos_s[b], jnp.int32)
    angles = pos_v[...].astype(F32) * freq_v[...]
    cos_a = jnp.cos(angles)
    sin_a = jnp.sin(angles)
    odd = lax.broadcasted_iota(jnp.int32, (ROWS, HD), 1) % 2 == 1
    sin_a = jnp.where(odd, sin_a, -sin_a)

    acc[...] = jnp.zeros_like(acc)

    def w_step(i, carry):
        for cp in w_copies(i):
            cp.wait()
        @pl.when(i >= KCH - LATE)
        def _():
            for u in range(NB // LATE):
                at = (i - (KCH - LATE)) * (NB // LATE) + u
                cache_copy(kc, k_v, sem_k, at).start()
                cache_copy(vc, v_v, sem_v, at).start()

        rows = pl.ds(pl.multiple_of(i * KSTEP, KSTEP), KSTEP)
        acc[...] += jnp.dot(n_v[:, rows], w_v[rows, :], preferred_element_type=F32)
        return carry

    lax.fori_loop(0, KCH, w_step, 0)

    def rotate(val):
        swapped = jnp.where(odd, pltpu.roll(val, 1, 1), pltpu.roll(val, HD - 1, 1))
        return (val * cos_a + swapped * sin_a).astype(BF16).astype(F32)

    for h in range(HEADS):
        qs[pl.ds(h, ROWS, stride=HEADS), :] = rotate(acc[:, h * HD:(h + 1) * HD])
    for h in range(KV):
        lo = (HEADS + h) * HD
        ks[pl.ds(h, ROWS, stride=KV), :] = rotate(acc[:, lo:lo + HD])
        lo = (HEADS + KV + h) * HD
        vs[pl.ds(h, ROWS, stride=KV), :] = acc[:, lo:lo + HD].astype(BF16).astype(F32)
    kn_ref[...] = ks[...].astype(BF16)
    vn_ref[...] = vs[...].astype(BF16)

    row16 = lax.broadcasted_iota(jnp.int32, (16, HD), 0)
    lane = lax.broadcasted_iota(jnp.int32, (HEADS, KV * BLK), 1)
    group = lax.broadcasted_iota(jnp.int32, (HEADS, KV * BLK), 0) // (HEADS // KV)
    same_head = (lane % KV) == group
    lane_slot = lane // KV
    stat_lane = lax.broadcasted_iota(jnp.int32, (HEADS, HD), 1)

    def put_new(cache_v, new, b, slot):
        inside = jnp.logical_and(slot >= 0, slot < BLK)
        tile = jnp.where(inside, slot // 8, 0)
        local = jnp.where(inside, slot - tile * 8, -1)
        at = pl.ds(pl.multiple_of(tile * 16, 16), 16)
        old = cache_v[b, at, :].astype(F32)
        both = jnp.where(row16 % 2 == 0, new[pl.ds(2 * b, 1), :], new[pl.ds(2 * b + 1, 1), :])
        cache_v[b, at, :] = jnp.where(row16 // 2 == local, both, old).astype(BF16)

    def chunk(i, stat):
        cache_copy(kc, k_v, sem_k, i).wait()
        cache_copy(vc, v_v, sem_v, i).wait()
        slots = [pos_s[i * BCH + u] - sp * BLK for u in range(BCH)]
        for u in range(BCH):
            put_new(k_v, ks, i * BCH + u, slots[u])
            put_new(v_v, vs, i * BCH + u, slots[u])
        cache_copy(k_v, ko, sem_ko, i).start()
        cache_copy(v_v, vo, sem_vo, i).start()
        raw = []
        for u in range(BCH):
            b = i * BCH + u
            q = qs[pl.ds(pl.multiple_of(b * HEADS, HEADS), HEADS), :].astype(BF16)
            raw.append(lax.dot_general(q, k_v[b], (((1,), (1,)), ((), ())), preferred_element_type=F32))
        for u in range(BCH):
            b = i * BCH + u
            valid = jnp.logical_and(same_head, lane_slot <= slots[u])
            score = jnp.where(valid, raw[u] * (HD ** -0.5), NEG)
            top = jnp.max(score, axis=-1, keepdims=True)
            prob = jnp.where(valid, jnp.exp(score - top), 0.0)
            total = jnp.sum(prob, axis=-1, keepdims=True)
            out = jnp.dot(prob.astype(BF16), v_v[b], preferred_element_type=F32)
            half = b // 32
            part_ref[half, pl.ds(pl.multiple_of((b - half * 32) * HEADS, HEADS), HEADS), :] = out
            stat = jnp.where(stat_lane == b, top, stat)
            stat = jnp.where(stat_lane == b + ROWS, total, stat)
        return stat

    stat = lax.fori_loop(0, NB, chunk, jnp.zeros((HEADS, HD), F32))
    part_ref[0, 256:264, :] = stat
    part_ref[1, 256:264, :] = pltpu.roll(stat, 96, 1)
    for i in range(NB):
        cache_copy(k_v, ko, sem_ko, i).wait()
        cache_copy(v_v, vo, sem_vo, i).wait()


def attend(new_pos, x, gain, freq, wq, wk, wv, kc, vc):
    cache = jax.ShapeDtypeStruct(kc.shape, BF16)
    new = jax.ShapeDtypeStruct((ROWS * KV, HD), BF16)
    return pl.pallas_call(
        attend_kernel,
        out_shape=(cache, cache, new, new, jax.ShapeDtypeStruct((2, 264, HD), F32)),
        in_specs=[ANY] * 9,
        out_specs=(ANY, ANY, VM, VM, VM),
        scratch_shapes=[
            pltpu.SMEM((ROWS,), jnp.int32),
            pltpu.VMEM((ROWS, DIM), BF16),
            pltpu.VMEM((DIM,), BF16),
            pltpu.VMEM((1, HD), F32),
            pltpu.VMEM((DIM, QKV), BF16),
            pltpu.VMEM(kc.shape, BF16),
            pltpu.VMEM(vc.shape, BF16),
            pltpu.VMEM((ROWS, DIM), BF16),
            pltpu.VMEM((ROWS, QKV), F32),
            pltpu.VMEM((ROWS, HD), jnp.int32),
            pltpu.VMEM((ROWS * HEADS, HD), F32),
            pltpu.VMEM((ROWS * KV, HD), F32),
            pltpu.VMEM((ROWS * KV, HD), F32),
            pltpu.SemaphoreType.DMA((4,)),
            pltpu.SemaphoreType.DMA((KCH, 3)),
            pltpu.SemaphoreType.DMA((NB,)),
            pltpu.SemaphoreType.DMA((NB,)),
            pltpu.SemaphoreType.DMA((NB,)),
            pltpu.SemaphoreType.DMA((NB,)),
        ],
        compiler_params=pltpu.CompilerParams(vmem_limit_bytes=ATTEND_VMEM),
        name="attend",
    )(new_pos, x, gain, freq, wq, wk, wv, kc, vc)


TP = 4
COLS = DIM // 4
HID = 896
HCH = HID // 128
RB = ROWS // TP
NC = 2
CW = COLS // NC


def mix_kernel(part_ref, x_hbm, gain_hbm, wo, wg, wu, wd, out_ref,
               xb_v, gain_v, wo_v, wgu_v, wd_v,
               pa, pb, pc, at_o, lhs_v, mm, rs_buf, hfull, n2, act, act_b, ofull,
               sem_l, sem_g, sem_d, cs, cr, rs_s, rs_r, az_s, az_r, ay_s, ay_r, ac_s, ac_r,
               my_s, my_r, mc_s, mc_r):
    dp = lax.axis_index('dp')
    z = lax.axis_index('tp')
    sp = lax.axis_index('sp')
    y = sp // 2
    c = sp % 2
    sp_y = (1 - y) * 2 + c
    sp_c = y * 2 + (1 - c)
    sp_yc = (1 - y) * 2 + (1 - c)
    dev_y = (dp, z, sp_y)
    dev_c = (dp, z, sp_c)
    dev_z = [None] + [(dp, lax.rem(z + d, TP), sp) for d in range(1, TP)]
    src_z = [z] + [lax.rem(z + TP - d, TP) for d in range(1, TP)]

    def col_at(s, j=0, width=COLS):
        return pl.ds(pl.multiple_of(s * COLS + j * width, 128), width)

    def row_at(zz):
        return pl.ds(pl.multiple_of(zz * RB, RB), RB)

    loads = [pltpu.make_async_copy(wo.at[:, col_at(sp)], wo_v, sem_l.at[0]),
             pltpu.make_async_copy(x_hbm.at[row_at(z), col_at(sp)], xb_v, sem_l.at[1]),
             pltpu.make_async_copy(gain_hbm, gain_v, sem_l.at[2])]
    for cp in loads:
        cp.start()

    def gu_copies(j):
        cols = pl.ds(pl.multiple_of(sp * HID + j * 128, 128), 128)
        return (pltpu.make_async_copy(wg.at[:, cols], wgu_v.at[j, :, pl.ds(0, 128)], sem_g.at[j, 0]),
                pltpu.make_async_copy(wu.at[:, cols], wgu_v.at[j, :, pl.ds(128, 128)], sem_g.at[j, 1]))

    for j in range(HCH):
        for cp in gu_copies(j):
            cp.start()
    order = [sp, sp_c, sp_y, sp_yc]
    d_copies = [pltpu.make_async_copy(wd.at[pl.ds(pl.multiple_of(s * HID, 128), HID), col_at(sp)],
                                      wd_v.at[i], sem_d.at[i]) for i, s in enumerate(order)]
    for cp in d_copies:
        cp.start()

    barrier = pltpu.get_barrier_semaphore()
    for dev in [dev_y, dev_c] + dev_z[1:]:
        pl.semaphore_signal(barrier, inc=1, device_id=dev, device_id_type=MESH)
    pl.semaphore_wait(barrier, 5)

    sends = []

    def push(src, dst, ssem, rsem, dev):
        cp = pltpu.make_async_remote_copy(src_ref=src, dst_ref=dst, send_sem=ssem, recv_sem=rsem,
                                          device_id=dev, device_id_type=MESH)
        cp.start()
        sends.append(cp)
        return cp

    lane = lax.broadcasted_iota(jnp.int32, (HEADS, HD), 1)

    def weights(s1, s2):
        top = jnp.maximum(s1, s2)
        a1 = jnp.exp(s1 - top)
        a2 = jnp.exp(s2 - top)
        total = a1 * pltpu.roll(s1, 64, 1) + a2 * pltpu.roll(s2, 64, 1)
        return top, a1, a2, total

    cp = push(part_ref.at[1 - c], pa, cs.at[0], cr.at[0], dev_c)
    cp.wait_recv()
    top, a1, a2, total = weights(part_ref[c, 256:264, :], pa[256:264, :])
    for i in range(32):
        r = slice(i * 8, i * 8 + 8)
        pb[r, :] = a1[:, i:i + 1] * part_ref[c, r, :] + a2[:, i:i + 1] * pa[r, :]
    pb[256:264, :] = jnp.where(lane < 64, top, pltpu.roll(total, 64, 1))
    cp = push(pb, pc, cs.at[1], cr.at[1], dev_y)
    cp.wait_recv()
    top, a1, a2, total = weights(pb[256:264, :], pc[256:264, :])
    a1 = a1 / total
    a2 = a2 / total
    half = pl.multiple_of(c * 256, 256)
    for i in range(32):
        r = slice(i * 8, i * 8 + 8)
        at_o[pl.ds(pl.multiple_of(half + i * 8, 8), 8), :] = a1[:, i:i + 1] * pb[r, :] + a2[:, i:i + 1] * pc[r, :]
    mine = at_o.at[pl.ds(half, 256)]
    cp = push(mine, mine, cs.at[2], cr.at[2], dev_c)
    cp.wait_recv()
    for h in range(HEADS):
        lhs_v[:, h * HD:(h + 1) * HD] = at_o[pl.ds(h, ROWS, stride=HEADS), :].astype(BF16)

    def scatter(stage, j):
        cols = pl.ds(j * CW, CW)
        for d in range(1, TP):
            zz = lax.rem(z + d, TP)
            push(mm.at[stage, row_at(zz), cols], rs_buf.at[stage, d - 1, :, cols],
                 rs_s.at[stage, j, d - 1], rs_r.at[stage, j, d - 1], dev_z[d])

    def gather(stage, base, full):
        def blk(s, d, j):
            return full.at[row_at(src_z[d]), col_at(s, 0, COLS) if False else pl.ds(
                pl.multiple_of(s * COLS + j * CW, 128), CW)]

        def wait_in(ref, sem):
            pltpu.make_async_copy(ref, ref, sem).wait()

        for j in range(NC):
            cols = slice(j * CW, (j + 1) * CW)
            val = base(cols) + mm[stage, row_at(z), cols]
            for d in range(1, TP):
                wait_in(rs_buf.at[stage, d - 1, :, pl.ds(j * CW, CW)], rs_r.at[stage, j, d - 1])
                val = val + rs_buf[stage, d - 1, :, cols]
            full[row_at(z), pl.ds(pl.multiple_of(sp * COLS + j * CW, 128), CW)] = val
            own = blk(sp, 0, j)
            for d in range(1, TP):
                push(own, own, az_s.at[stage, j, d - 1], az_r.at[stage, j, d - 1], dev_z[d])
            push(own, own, ay_s.at[stage, j, 0], ay_r.at[stage, j, 0], dev_y)
            push(own, own, ac_s.at[stage, j, 0], ac_r.at[stage, j, 0], dev_c)
        for j in range(NC):
            for d in (1, 3, 2):
                ref = blk(sp, d, j)
                wait_in(ref, az_r.at[stage, j, d - 1])
                push(ref, ref, ay_s.at[stage, j, d], ay_r.at[stage, j, d], dev_y)
                push(ref, ref, ac_s.at[stage, j, d], ac_r.at[stage, j, d], dev_c)
        for j in range(NC):
            for d in (0, 1, 3, 2):
                ref = blk(sp_y, d, j)
                wait_in(ref, ay_r.at[stage, j, d])
                push(ref, ref, ac_s.at[stage, j, TP + d], ac_r.at[stage, j, TP + d], dev_c)
        for j in range(NC):
            for d in range(TP):
                wait_in(blk(sp_c, d, j), ac_r.at[stage, j, d])
                wait_in(blk(sp_yc, d, j), ac_r.at[stage, j, TP + d])

    for cp in loads:
        cp.wait()
    for j in range(NC):
        cols = slice(j * CW, (j + 1) * CW)
        mm[0, :, cols] = jnp.dot(lhs_v[...], wo_v[:, cols], preferred_element_type=F32)
        scatter(0, j)
    gather(0, lambda cols: xb_v[:, cols].astype(F32), hfull)

    for r in range(0, ROWS, 16):
        h = hfull[r:r + 16, :]
        inv = lax.rsqrt(jnp.mean(h * h, axis=-1, keepdims=True) + 1e-5)
        n2[r:r + 16, :] = (h * inv * gain_v[...].astype(F32).reshape(1, DIM)).astype(BF16)

    def act_copies(j):
        own = act.at[sp, j]
        return (pltpu.make_async_remote_copy(src_ref=own, dst_ref=own, send_sem=my_s.at[j], recv_sem=my_r.at[j],
                                             device_id=dev_y, device_id_type=MESH),
                pltpu.make_async_remote_copy(src_ref=own, dst_ref=own, send_sem=mc_s.at[0, j], recv_sem=mc_r.at[0, j],
                                             device_id=dev_c, device_id_type=MESH))

    def fwd_copy(j):
        ref = act.at[sp_y, j]
        return pltpu.make_async_remote_copy(src_ref=ref, dst_ref=ref, send_sem=mc_s.at[1, j], recv_sem=mc_r.at[1, j],
                                            device_id=dev_c, device_id_type=MESH)

    def hidden_step(j, carry):
        for cp in gu_copies(j):
            cp.wait()
        gu = jnp.dot(n2[...], wgu_v[j], preferred_element_type=F32)
        gate = gu[:, :128]
        val = gate * jax.nn.sigmoid(gate) * gu[:, 128:]
        act[sp, j] = val.astype(BF16).astype(F32)
        for cp in act_copies(j):
            cp.start()
        return carry

    lax.fori_loop(0, HCH, hidden_step, 0)

    def down(i, s):
        for j in range(HCH):
            act_b[:, j * 128:(j + 1) * 128] = act[s, j].astype(BF16)
        d_copies[i].wait()
        for k in range(0, COLS, 256):
            prod = jnp.dot(act_b[...], wd_v[i, :, k:k + 256], preferred_element_type=F32)
            if i == 0:
                mm[1, :, k:k + 256] = prod
            else:
                mm[1, :, k:k + 256] += prod

    down(0, sp)
    for j in range(HCH):
        act_copies(j)[1].wait_recv()
    down(1, sp_c)
    for j in range(HCH):
        act_copies(j)[0].wait_recv()
        fwd_copy(j).start()
    down(2, sp_y)
    for j in range(HCH):
        fwd_copy(j).wait_recv()
    down(3, sp_yc)
    for j in range(NC):
        scatter(1, j)

    own_h = hfull.at[row_at(z), col_at(sp)]
    gather(1, lambda cols: own_h[:, cols], ofull)
    out_ref[...] = ofull[...].astype(BF16)

    for cp in sends:
        cp.wait_send()
    for j in range(HCH):
        for cp in act_copies(j):
            cp.wait_send()
        fwd_copy(j).wait_send()


def mix(part, x, gain, wo, wg, wu, wd):
    dma = pltpu.SemaphoreType.DMA
    return pl.pallas_call(
        mix_kernel,
        out_shape=jax.ShapeDtypeStruct((ROWS, DIM), BF16),
        in_specs=[VM] + [ANY] * 6,
        out_specs=VM,
        scratch_shapes=[
            pltpu.VMEM((RB, COLS), BF16),
            pltpu.VMEM((DIM,), BF16),
            pltpu.VMEM((1024, COLS), BF16),
            pltpu.VMEM((HCH, DIM, 256), BF16),
            pltpu.VMEM((4, HID, COLS), BF16),
            pltpu.VMEM((264, HD), F32),
            pltpu.VMEM((264, HD), F32),
            pltpu.VMEM((264, HD), F32),
            pltpu.VMEM((ROWS * HEADS, HD), F32),
            pltpu.VMEM((ROWS, 1024), BF16),
            pltpu.VMEM((2, ROWS, COLS), F32),
            pltpu.VMEM((2, TP - 1, RB, COLS), F32),
            pltpu.VMEM((ROWS, DIM), F32),
            pltpu.VMEM((ROWS, DIM), BF16),
            pltpu.VMEM((4, HCH, ROWS, 128), F32),
            pltpu.VMEM((ROWS, HID), BF16),
            pltpu.VMEM((ROWS, DIM), F32),
            dma((3,)), dma((HCH, 2)), dma((4,)),
            dma((3,)), dma((3,)),
            dma((2, NC, 3)), dma((2, NC, 3)),
            dma((2, NC, 3)), dma((2, NC, 3)),
            dma((2, NC, TP)), dma((2, NC, TP)),
            dma((2, NC, 2 * TP)), dma((2, NC, 2 * TP)),
            dma((HCH,)), dma((HCH,)),
            dma((2, HCH)), dma((2, HCH)),
        ],
        compiler_params=pltpu.CompilerParams(vmem_limit_bytes=MIX_VMEM, collective_id=0, has_side_effects=True),
        name="mix",
    )(part, x, gain, wo, wg, wu, wd)


def solution(mesh):
    def local_step(layer_in, new_pos, k_blk, v_blk, attn_gain, w_query, w_key, w_value, w_out, mlp_gain, w_gate, w_up, w_down):
        half_idx = np.arange(HD // 2, dtype=np.float32)
        inv_freq = (1.0 / (np.float32(ROPE_THETA) ** (np.float32(2.0) * half_idx / np.float32(HD)))).astype(np.float32)
        freq = jnp.asarray(np.repeat(inv_freq, 2)[None, :])
        flat = (ROWS, BLK * KV, HD)
        k_out, v_out, k_new, v_new, part = attend(
            new_pos, layer_in, attn_gain, freq, w_query, w_key, w_value,
            k_blk.reshape(flat), v_blk.reshape(flat))
        layer_out = mix(part, layer_in, mlp_gain, w_out, w_gate, w_up, w_down)
        return (layer_out, k_out.reshape(k_blk.shape), v_out.reshape(v_blk.shape),
                k_new.reshape(ROWS, KV, HD), v_new.reshape(ROWS, KV, HD))

    cache_spec = P('dp', 'sp', 'tp', None)
    new_spec = P('dp', 'tp', None)
    in_specs = (P('dp', None), P('dp'), cache_spec, cache_spec, P(None), P(None, 'tp'), P(None, 'tp'), P(None, 'tp'), P('tp', None), P(None), P(None, 'tp'), P(None, 'tp'), P('tp', None))
    out_specs = (P('dp', None), cache_spec, cache_spec, new_spec, new_spec)
    return jax.shard_map(local_step, mesh=mesh, in_specs=in_specs, out_specs=out_specs, check_vma=False)
```

```python
import functools

import jax
import jax.numpy as jnp
import numpy as np
from jax import lax
from jax.experimental import pallas as pl
from jax.experimental.pallas import tpu as pltpu
from jax.sharding import PartitionSpec as P

ROPE_THETA = 1000000
MESH = pl.DeviceIdType.MESH
F32 = jnp.float32
BF16 = jnp.bfloat16
NEG = float(np.finfo(np.float32).min)
ATTEND_VMEM = 62 * 1024 * 1024
MIX_VMEM = 48 * 1024 * 1024
ANY = pl.BlockSpec(memory_space=pltpu.HBM)
VM = pl.BlockSpec(memory_space=pltpu.VMEM)

ROWS = 64
DIM = 5120
HD = 128
HEADS = 8
KV = 2
BLK = 128
QKV = (HEADS + 2 * KV) * HD
KSTEP = 1024
KCH = DIM // KSTEP
BCH = 16
NB = ROWS // BCH
QROWS = BCH * HEADS
LATE = 4


def attend_kernel(pos_hbm, x_hbm, gain_hbm, freq_hbm, wq, wk, wv, kc, vc,
                  ko, vo, kn_ref, vn_ref, part_ref,
                  pos_s, x_v, gain_v, freq_v, w_v, k_v, v_v, n_v, acc, pos_v, qs, ks, vs, kn_v, vn_v,
                  sem_m, sem_w, sem_k, sem_v, sem_ko, sem_vo, sem_n):
    sp = lax.axis_index('sp')

    small = [pltpu.make_async_copy(pos_hbm, pos_s, sem_m.at[0]),
             pltpu.make_async_copy(x_hbm, x_v, sem_m.at[1]),
             pltpu.make_async_copy(gain_hbm, gain_v, sem_m.at[2]),
             pltpu.make_async_copy(freq_hbm, freq_v, sem_m.at[3])]
    for cp in small:
        cp.start()

    def w_copies(i):
        rows = pl.ds(pl.multiple_of(i * KSTEP, KSTEP), KSTEP)
        return (pltpu.make_async_copy(wq.at[rows], w_v.at[rows, pl.ds(0, 1024)], sem_w.at[i, 0]),
                pltpu.make_async_copy(wk.at[rows], w_v.at[rows, pl.ds(1024, 256)], sem_w.at[i, 1]),
                pltpu.make_async_copy(wv.at[rows], w_v.at[rows, pl.ds(1280, 256)], sem_w.at[i, 2]))

    def cache_copy(src, dst, sem, i):
        rows = pl.ds(pl.multiple_of(i * BCH, BCH), BCH)
        return pltpu.make_async_copy(src.at[rows], dst.at[rows], sem.at[i])

    for i in range(KCH):
        for cp in w_copies(i):
            cp.start()
    for cp in small:
        cp.wait()
    for r in range(0, ROWS, 16):
        x = x_v[r:r + 16, :].astype(F32)
        inv = lax.rsqrt(jnp.mean(x * x, axis=-1, keepdims=True) + 1e-5)
        n_v[r:r + 16, :] = (x * inv * gain_v[...].astype(F32).reshape(1, DIM)).astype(BF16)
    for b in range(ROWS):
        pos_v[b:b + 1, :] = jnp.full((1, HD), pos_s[b], jnp.int32)
    angles = pos_v[...].astype(F32) * freq_v[...]
    cos_a = jnp.cos(angles)
    sin_a = jnp.sin(angles)
    odd = lax.broadcasted_iota(jnp.int32, (ROWS, HD), 1) % 2 == 1
    sin_a = jnp.where(odd, sin_a, -sin_a)

    acc[...] = jnp.zeros_like(acc)

    def w_step(i, carry):
        for cp in w_copies(i):
            cp.wait()
        @pl.when(i >= KCH - LATE)
        def _():
            for u in range(NB // LATE):
                at = (i - (KCH - LATE)) * (NB // LATE) + u
                cache_copy(kc, k_v, sem_k, at).start()
                cache_copy(vc, v_v, sem_v, at).start()

        rows = pl.ds(pl.multiple_of(i * KSTEP, KSTEP), KSTEP)
        acc[...] += jnp.dot(n_v[:, rows], w_v[rows, :], preferred_element_type=F32)
        return carry

    lax.fori_loop(0, KCH, w_step, 0)

    def rotate(val):
        swapped = jnp.where(odd, pltpu.roll(val, 1, 1), pltpu.roll(val, HD - 1, 1))
        return (val * cos_a + swapped * sin_a).astype(BF16).astype(F32)

    for h in range(HEADS):
        qs[pl.ds(h, ROWS, stride=HEADS), :] = rotate(acc[:, h * HD:(h + 1) * HD])
    for h in range(KV):
        lo = (HEADS + h) * HD
        ks[pl.ds(h, ROWS, stride=KV), :] = rotate(acc[:, lo:lo + HD])
        lo = (HEADS + KV + h) * HD
        vs[pl.ds(h, ROWS, stride=KV), :] = acc[:, lo:lo + HD].astype(BF16).astype(F32)
    kn_v[...] = ks[...].astype(BF16)
    vn_v[...] = vs[...].astype(BF16)
    new_copies = [pltpu.make_async_copy(kn_v, kn_ref, sem_n.at[0]), pltpu.make_async_copy(vn_v, vn_ref, sem_n.at[1])]
    for cp in new_copies:
        cp.start()

    row16 = lax.broadcasted_iota(jnp.int32, (16, HD), 0)
    lane = lax.broadcasted_iota(jnp.int32, (HEADS, KV * BLK), 1)
    group = lax.broadcasted_iota(jnp.int32, (HEADS, KV * BLK), 0) // (HEADS // KV)
    same_head = (lane % KV) == group
    lane_slot = lane // KV
    stat_lane = lax.broadcasted_iota(jnp.int32, (HEADS, HD), 1)

    def put_new(cache_v, new, b, slot):
        inside = jnp.logical_and(slot >= 0, slot < BLK)
        tile = jnp.where(inside, slot // 8, 0)
        local = jnp.where(inside, slot - tile * 8, -1)
        at = pl.ds(pl.multiple_of(tile * 16, 16), 16)
        old = cache_v[b, at, :].astype(F32)
        both = jnp.where(row16 % 2 == 0, new[pl.ds(2 * b, 1), :], new[pl.ds(2 * b + 1, 1), :])
        cache_v[b, at, :] = jnp.where(row16 // 2 == local, both, old).astype(BF16)

    for i in range(NB):
        cache_copy(kc, k_v, sem_k, i).wait()
        cache_copy(vc, v_v, sem_v, i).wait()
        slots = [pos_s[i * BCH + u] - sp * BLK for u in range(BCH)]
        for u in range(BCH):
            put_new(k_v, ks, i * BCH + u, slots[u])
            put_new(v_v, vs, i * BCH + u, slots[u])
        cache_copy(k_v, ko, sem_ko, i).start()
        cache_copy(v_v, vo, sem_vo, i).start()
        raw = []
        for u in range(BCH):
            b = i * BCH + u
            q = qs[b * HEADS:(b + 1) * HEADS, :].astype(BF16)
            raw.append(lax.dot_general(q, k_v[b], (((1,), (1,)), ((), ())), preferred_element_type=F32))
        stat = jnp.zeros((HEADS, HD), F32)
        for u in range(BCH):
            b = i * BCH + u
            valid = jnp.logical_and(same_head, lane_slot <= slots[u])
            score = jnp.where(valid, raw[u] * (HD ** -0.5), NEG)
            top = jnp.max(score, axis=-1, keepdims=True)
            prob = jnp.where(valid, jnp.exp(score - top), 0.0)
            total = jnp.sum(prob, axis=-1, keepdims=True)
            part_ref[i, u * HEADS:(u + 1) * HEADS, :] = jnp.dot(prob.astype(BF16), v_v[b], preferred_element_type=F32)
            stat = jnp.where(stat_lane == u, top, stat)
            stat = jnp.where(stat_lane == u + 64, total, stat)
        part_ref[i, QROWS:QROWS + HEADS, :] = stat
    for i in range(NB):
        cache_copy(k_v, ko, sem_ko, i).wait()
        cache_copy(v_v, vo, sem_vo, i).wait()
    for cp in new_copies:
        cp.wait()


def attend(new_pos, x, gain, freq, wq, wk, wv, kc, vc):
    cache = jax.ShapeDtypeStruct(kc.shape, BF16)
    new = jax.ShapeDtypeStruct((ROWS * KV, HD), BF16)
    return pl.pallas_call(
        attend_kernel,
        out_shape=(cache, cache, new, new, jax.ShapeDtypeStruct((NB, QROWS + HEADS, HD), F32)),
        in_specs=[ANY] * 9,
        out_specs=(ANY,) * 4 + (VM,),
        scratch_shapes=[
            pltpu.SMEM((ROWS,), jnp.int32),
            pltpu.VMEM((ROWS, DIM), BF16),
            pltpu.VMEM((DIM,), BF16),
            pltpu.VMEM((1, HD), F32),
            pltpu.VMEM((DIM, QKV), BF16),
            pltpu.VMEM(kc.shape, BF16),
            pltpu.VMEM(vc.shape, BF16),
            pltpu.VMEM((ROWS, DIM), BF16),
            pltpu.VMEM((ROWS, QKV), F32),
            pltpu.VMEM((ROWS, HD), jnp.int32),
            pltpu.VMEM((ROWS * HEADS, HD), F32),
            pltpu.VMEM((ROWS * KV, HD), F32),
            pltpu.VMEM((ROWS * KV, HD), F32),
            pltpu.VMEM((ROWS * KV, HD), BF16),
            pltpu.VMEM((ROWS * KV, HD), BF16),
            pltpu.SemaphoreType.DMA((4,)),
            pltpu.SemaphoreType.DMA((KCH, 3)),
            pltpu.SemaphoreType.DMA((NB,)),
            pltpu.SemaphoreType.DMA((NB,)),
            pltpu.SemaphoreType.DMA((NB,)),
            pltpu.SemaphoreType.DMA((NB,)),
            pltpu.SemaphoreType.DMA((2,)),
        ],
        compiler_params=pltpu.CompilerParams(vmem_limit_bytes=ATTEND_VMEM),
        name="attend",
    )(new_pos, x, gain, freq, wq, wk, wv, kc, vc)


TP = 4
COLS = DIM // 4
HID = 896
HCH = HID // 128
RB = ROWS // TP
CHUNKS = ((0, 512), (512, 768))
NC = len(CHUNKS)


def mix_kernel(part_ref, x_hbm, gain_hbm, wo, wg, wu, wd, out_ref,
               xb_v, gain_v, wo_v, wgu_v, wd_v,
               pa, pb, pc, at_o, lhs_v, mm, rs_buf, hfull, n2, act, act_b, ofull,
               sem_l, sem_g, sem_d, cs, cr, rs_s, rs_r, az_s, az_r, ay_s, ay_r, ac_s, ac_r,
               my_s, my_r, mc_s, mc_r, zr, gu_v):
    dp = lax.axis_index('dp')
    z = lax.axis_index('tp')
    sp = lax.axis_index('sp')
    y = sp // 2
    c = sp % 2
    sp_y = (1 - y) * 2 + c
    sp_c = y * 2 + (1 - c)
    sp_yc = (1 - y) * 2 + (1 - c)
    dev_y = (dp, z, sp_y)
    dev_c = (dp, z, sp_c)
    dev_z = [None] + [(dp, lax.rem(z + d, TP), sp) for d in range(1, TP)]
    src_z = [z] + [lax.rem(z + TP - d, TP) for d in range(1, TP)]

    def col_at(s):
        return pl.ds(pl.multiple_of(s * COLS, 128), COLS)

    def chunk_at(s, j):
        return pl.ds(pl.multiple_of(s * COLS + CHUNKS[j][0], 128), CHUNKS[j][1])

    def row_at(zz):
        return pl.ds(pl.multiple_of(zz * RB, RB), RB)

    loads = [pltpu.make_async_copy(wo.at[:, col_at(sp)], wo_v, sem_l.at[0]),
             pltpu.make_async_copy(x_hbm.at[row_at(z), col_at(sp)], xb_v, sem_l.at[1]),
             pltpu.make_async_copy(gain_hbm, gain_v, sem_l.at[2])]
    for cp in loads:
        cp.start()

    def gu_copies(j):
        cols = pl.ds(pl.multiple_of(sp * HID + j * 128, 128), 128)
        return (pltpu.make_async_copy(wg.at[:, cols], wgu_v.at[j, :, pl.ds(0, 128)], sem_g.at[j, 0]),
                pltpu.make_async_copy(wu.at[:, cols], wgu_v.at[j, :, pl.ds(128, 128)], sem_g.at[j, 1]))

    for j in range(HCH):
        for cp in gu_copies(j):
            cp.start()
    order = [sp, sp_c, sp_y, sp_yc]
    d_copies = [pltpu.make_async_copy(wd.at[pl.ds(pl.multiple_of(s * HID, 128), HID), col_at(sp)],
                                      wd_v.at[i], sem_d.at[i]) for i, s in enumerate(order)]
    for cp in d_copies:
        cp.start()

    has_l, has_r = z > 0, z < TP - 1
    dev_l = (dp, jnp.maximum(z - 1, 0), sp)
    dev_r = (dp, jnp.minimum(z + 1, TP - 1), sp)

    def signal(sem, dev, cond=None):
        if cond is None:
            pl.semaphore_signal(sem, inc=1, device_id=dev, device_id_type=MESH)
        else:
            @pl.when(cond)
            def _():
                pl.semaphore_signal(sem, inc=1, device_id=dev, device_id_type=MESH)

    def wait_if(sem, cond):
        @pl.when(cond)
        def _():
            pl.semaphore_wait(sem, 1)

    barrier = pltpu.get_barrier_semaphore()
    signal(barrier, dev_y)
    signal(barrier, dev_c)
    signal(barrier, dev_l, has_l)
    signal(barrier, dev_r, has_r)
    pl.semaphore_wait(barrier, 2 + has_l.astype(jnp.int32) + has_r.astype(jnp.int32))
    inner = jnp.logical_and(has_l, has_r)
    signal(zr.at[0], dev_l, inner)
    signal(zr.at[1], dev_r, inner)

    sends = []

    def push(src, dst, ssem, rsem, dev):
        cp = pltpu.make_async_remote_copy(src_ref=src, dst_ref=dst, send_sem=ssem, recv_sem=rsem,
                                          device_id=dev, device_id_type=MESH)
        cp.start()
        sends.append(cp)
        return cp

    lane = lax.broadcasted_iota(jnp.int32, (HEADS, HD), 1)

    def weights(s1, s2):
        top = jnp.maximum(s1, s2)
        a1 = jnp.exp(s1 - top)
        a2 = jnp.exp(s2 - top)
        total = a1 * pltpu.roll(s1, 64, 1) + a2 * pltpu.roll(s2, 64, 1)
        return top, a1, a2, total

    half = pl.multiple_of(c * 256, 256)
    st = slice(QROWS, QROWS + HEADS)
    first = [push(part_ref.at[(1 - c) * 2 + k], pa.at[k], cs.at[0, k], cr.at[0, k], dev_c) for k in range(2)]
    second = []
    for k in range(2):
        first[k].wait_recv()
        mine = part_ref.at[c * 2 + k]
        top, a1, a2, total = weights(mine[st, :], pa[k, st, :])
        for i in range(BCH):
            r = slice(i * 8, i * 8 + 8)
            pb[k, r, :] = a1[:, i:i + 1] * mine[r, :] + a2[:, i:i + 1] * pa[k, r, :]
        pb[k, st, :] = jnp.where(lane < 64, top, pltpu.roll(total, 64, 1))
        second.append(push(pb.at[k], pc.at[k], cs.at[1, k], cr.at[1, k], dev_y))
    wait_if(zr.at[0], z + 2 < TP)
    wait_if(zr.at[1], z - 2 >= 0)
    signal(zr.at[2], dev_l, z == 1)
    signal(zr.at[3], dev_r, z == 2)
    third = []
    for k in range(2):
        second[k].wait_recv()
        top, a1, a2, total = weights(pb[k, st, :], pc[k, st, :])
        a1 = a1 / total
        a2 = a2 / total
        for i in range(BCH):
            r = slice(i * 8, i * 8 + 8)
            to = pl.ds(pl.multiple_of(half + k * QROWS + i * 8, 8), 8)
            at_o[to, :] = a1[:, i:i + 1] * pb[k, r, :] + a2[:, i:i + 1] * pc[k, r, :]
        piece = at_o.at[pl.ds(pl.multiple_of(half + k * QROWS, QROWS), QROWS)]
        third.append(push(piece, piece, cs.at[2, k], cr.at[2, k], dev_c))
    for cp in third:
        cp.wait_recv()
    wait_if(zr.at[2], z == 0)
    wait_if(zr.at[3], z == TP - 1)
    for h in range(HEADS):
        lhs_v[:, h * HD:(h + 1) * HD] = at_o[pl.ds(h, ROWS, stride=HEADS), :].astype(BF16)

    def scatter(stage, j):
        cols = pl.ds(*CHUNKS[j])
        for d in range(1, TP):
            zz = lax.rem(z + d, TP)
            push(mm.at[stage, row_at(zz), cols], rs_buf.at[stage, d - 1, :, cols],
                 rs_s.at[stage, j, d - 1], rs_r.at[stage, j, d - 1], dev_z[d])

    def gather(stage, base, full):
        def blk(s, d, j):
            return full.at[row_at(src_z[d]), chunk_at(s, j)]

        def wait_in(ref, sem):
            pltpu.make_async_copy(ref, ref, sem).wait()

        for j in range(NC):
            cols = pl.ds(*CHUNKS[j])
            val = base(cols) + mm[stage, row_at(z), cols]
            for d in range(1, TP):
                wait_in(rs_buf.at[stage, d - 1, :, cols], rs_r.at[stage, j, d - 1])
                val = val + rs_buf[stage, d - 1, :, cols]
            full[row_at(z), chunk_at(sp, j)] = val
            own = blk(sp, 0, j)
            for d in range(1, TP):
                push(own, own, az_s.at[stage, j, d - 1], az_r.at[stage, j, d - 1], dev_z[d])
            push(own, own, ay_s.at[stage, j, 0], ay_r.at[stage, j, 0], dev_y)
            push(own, own, ac_s.at[stage, j, 0], ac_r.at[stage, j, 0], dev_c)
        for j in range(NC):
            for d in (1, 3, 2):
                ref = blk(sp, d, j)
                wait_in(ref, az_r.at[stage, j, d - 1])
                push(ref, ref, ay_s.at[stage, j, d], ay_r.at[stage, j, d], dev_y)
                push(ref, ref, ac_s.at[stage, j, d], ac_r.at[stage, j, d], dev_c)
        for j in range(NC):
            for d in (0, 1, 3, 2):
                ref = blk(sp_y, d, j)
                wait_in(ref, ay_r.at[stage, j, d])
                push(ref, ref, ac_s.at[stage, j, TP + d], ac_r.at[stage, j, TP + d], dev_c)
        for j in range(NC):
            for d in range(TP):
                wait_in(blk(sp_c, d, j), ac_r.at[stage, j, d])
                wait_in(blk(sp_yc, d, j), ac_r.at[stage, j, TP + d])

    for cp in loads:
        cp.wait()
    for j in range(NC):
        cols = pl.ds(*CHUNKS[j])
        mm[0, :, cols] = jnp.dot(lhs_v[...], wo_v[:, cols], preferred_element_type=F32)
        scatter(0, j)
    gather(0, lambda cols: xb_v[:, cols].astype(F32), hfull)

    for r in range(0, ROWS, 16):
        h = hfull[r:r + 16, :]
        inv = lax.rsqrt(jnp.mean(h * h, axis=-1, keepdims=True) + 1e-5)
        n2[r:r + 16, :] = (h * inv * gain_v[...].astype(F32).reshape(1, DIM)).astype(BF16)

    def act_copies(j):
        own = act.at[sp, j]
        return (pltpu.make_async_remote_copy(src_ref=own, dst_ref=own, send_sem=my_s.at[j], recv_sem=my_r.at[j],
                                             device_id=dev_y, device_id_type=MESH),
                pltpu.make_async_remote_copy(src_ref=own, dst_ref=own, send_sem=mc_s.at[0, j], recv_sem=mc_r.at[0, j],
                                             device_id=dev_c, device_id_type=MESH))

    def fwd_copy(j):
        ref = act.at[sp_y, j]
        return pltpu.make_async_remote_copy(src_ref=ref, dst_ref=ref, send_sem=mc_s.at[1, j], recv_sem=mc_r.at[1, j],
                                            device_id=dev_c, device_id_type=MESH)

    def hidden_dot(j):
        for cp in gu_copies(j):
            cp.wait()
        gu_v[j % 2] = jnp.dot(n2[...], wgu_v[j], preferred_element_type=F32)

    def hidden_act(j):
        gate = gu_v[j % 2, :, :128]
        val = gate * jax.nn.sigmoid(gate) * gu_v[j % 2, :, 128:]
        act[sp, j] = val.astype(BF16).astype(F32)
        for cp in act_copies(j):
            cp.start()

    hidden_dot(0)
    for j in range(1, HCH):
        hidden_dot(j)
        hidden_act(j - 1)
    hidden_act(HCH - 1)

    def down(i, s):
        for j in range(HCH):
            act_b[:, j * 128:(j + 1) * 128] = act[s, j].astype(BF16)
        d_copies[i].wait()
        for k in range(0, COLS, 256):
            prod = jnp.dot(act_b[...], wd_v[i, :, k:k + 256], preferred_element_type=F32)
            if i == 0:
                mm[1, :, k:k + 256] = prod
            else:
                mm[1, :, k:k + 256] += prod
            if i == 3:
                for j in range(NC):
                    if CHUNKS[j][0] + CHUNKS[j][1] == k + 256:
                        scatter(1, j)

    down(0, sp)
    for j in range(HCH):
        act_copies(j)[1].wait_recv()
    down(1, sp_c)
    for j in range(HCH):
        act_copies(j)[0].wait_recv()
        fwd_copy(j).start()
    down(2, sp_y)
    for j in range(HCH):
        fwd_copy(j).wait_recv()
    down(3, sp_yc)

    own_h = hfull.at[row_at(z), col_at(sp)]
    gather(1, lambda cols: own_h[:, cols], ofull)
    out_ref[...] = ofull[...].astype(BF16)

    for cp in sends:
        cp.wait_send()
    for j in range(HCH):
        for cp in act_copies(j):
            cp.wait_send()
        fwd_copy(j).wait_send()


def mix(part, x, gain, wo, wg, wu, wd):
    dma = pltpu.SemaphoreType.DMA
    return pl.pallas_call(
        mix_kernel,
        out_shape=jax.ShapeDtypeStruct((ROWS, DIM), BF16),
        in_specs=[VM] + [ANY] * 6,
        out_specs=VM,
        scratch_shapes=[
            pltpu.VMEM((RB, COLS), BF16),
            pltpu.VMEM((DIM,), BF16),
            pltpu.VMEM((1024, COLS), BF16),
            pltpu.VMEM((HCH, DIM, 256), BF16),
            pltpu.VMEM((4, HID, COLS), BF16),
            pltpu.VMEM((2, QROWS + HEADS, HD), F32),
            pltpu.VMEM((2, QROWS + HEADS, HD), F32),
            pltpu.VMEM((2, QROWS + HEADS, HD), F32),
            pltpu.VMEM((ROWS * HEADS, HD), F32),
            pltpu.VMEM((ROWS, 1024), BF16),
            pltpu.VMEM((2, ROWS, COLS), F32),
            pltpu.VMEM((2, TP - 1, RB, COLS), F32),
            pltpu.VMEM((ROWS, DIM), F32),
            pltpu.VMEM((ROWS, DIM), BF16),
            pltpu.VMEM((4, HCH, ROWS, 128), F32),
            pltpu.VMEM((ROWS, HID), BF16),
            pltpu.VMEM((ROWS, DIM), F32),
            dma((3,)), dma((HCH, 2)), dma((4,)),
            dma((3, 2)), dma((3, 2)),
            dma((2, NC, 3)), dma((2, NC, 3)),
            dma((2, NC, 3)), dma((2, NC, 3)),
            dma((2, NC, TP)), dma((2, NC, TP)),
            dma((2, NC, 2 * TP)), dma((2, NC, 2 * TP)),
            dma((HCH,)), dma((HCH,)),
            dma((2, HCH)), dma((2, HCH)),
            pltpu.SemaphoreType.REGULAR((4,)),
            pltpu.VMEM((2, ROWS, 256), F32),
        ],
        compiler_params=pltpu.CompilerParams(vmem_limit_bytes=MIX_VMEM, collective_id=0, has_side_effects=True),
        name="mix",
    )(part, x, gain, wo, wg, wu, wd)


def solution(mesh):
    def local_step(layer_in, new_pos, k_blk, v_blk, attn_gain, w_query, w_key, w_value, w_out, mlp_gain, w_gate, w_up, w_down):
        half_idx = np.arange(HD // 2, dtype=np.float32)
        inv_freq = (1.0 / (np.float32(ROPE_THETA) ** (np.float32(2.0) * half_idx / np.float32(HD)))).astype(np.float32)
        freq = jnp.asarray(np.repeat(inv_freq, 2)[None, :])
        flat = (ROWS, BLK * KV, HD)
        k_out, v_out, k_new, v_new, part = attend(
            new_pos, layer_in, attn_gain, freq, w_query, w_key, w_value,
            k_blk.reshape(flat), v_blk.reshape(flat))
        layer_out = mix(part, layer_in, mlp_gain, w_out, w_gate, w_up, w_down)
        return (layer_out, k_out.reshape(k_blk.shape), v_out.reshape(v_blk.shape),
                k_new.reshape(ROWS, KV, HD), v_new.reshape(ROWS, KV, HD))

    cache_spec = P('dp', 'sp', 'tp', None)
    new_spec = P('dp', 'tp', None)
    in_specs = (P('dp', None), P('dp'), cache_spec, cache_spec, P(None), P(None, 'tp'), P(None, 'tp'), P(None, 'tp'), P('tp', None), P(None), P(None, 'tp'), P(None, 'tp'), P('tp', None))
    out_specs = (P('dp', None), cache_spec, cache_spec, new_spec, new_spec)
    return jax.shard_map(local_step, mesh=mesh, in_specs=in_specs, out_specs=out_specs, check_vma=False)
```

```python
import functools

import jax
import jax.numpy as jnp
import numpy as np
from jax import lax
from jax.experimental import pallas as pl
from jax.experimental.pallas import tpu as pltpu
from jax.sharding import PartitionSpec as P

ROPE_THETA = 1000000
MESH = pl.DeviceIdType.MESH
F32 = jnp.float32
BF16 = jnp.bfloat16
NEG = float(np.finfo(np.float32).min)
ATTEND_VMEM = 48 * 1024 * 1024
MIX_VMEM = 48 * 1024 * 1024
ANY = pl.BlockSpec(memory_space=pltpu.HBM)
VM = pl.BlockSpec(memory_space=pltpu.VMEM)

HALF_IDX = np.arange(64, dtype=np.float32)
INV_FREQ = np.float32(1.0) / (np.float32(ROPE_THETA) ** (np.float32(2.0) * HALF_IDX / np.float32(128)))

ROWS = 64
DIM = 5120
HD = 128
HEADS = 8
KV = 2
BLK = 128
QKV = (HEADS + 2 * KV) * HD
KSTEP = 1024
KCH = DIM // KSTEP
BCH = 16
NB = ROWS // BCH
QROWS = BCH * HEADS


def attend_kernel(pos_hbm, x_hbm, gain_hbm, wq, wk, wv, kc, vc,
                  ko, vo, kn_ref, vn_ref, part_ref,
                  pos_s, x_v, gain_v, w_v, k_v, v_v, n_v, acc, pos_v, qs, ks, vs, kn_v, vn_v,
                  sem_m, sem_w, sem_k, sem_v, sem_ko, sem_vo, sem_n):
    sp = lax.axis_index('sp')

    small = [pltpu.make_async_copy(pos_hbm, pos_s, sem_m.at[0]),
             pltpu.make_async_copy(x_hbm, x_v, sem_m.at[1]),
             pltpu.make_async_copy(gain_hbm, gain_v, sem_m.at[2])]
    for cp in small:
        cp.start()

    def w_copies(i):
        rows = pl.ds(pl.multiple_of(i * KSTEP, KSTEP), KSTEP)
        return (pltpu.make_async_copy(wq.at[rows], w_v.at[rows, pl.ds(0, 1024)], sem_w.at[i, 0]),
                pltpu.make_async_copy(wk.at[rows], w_v.at[rows, pl.ds(1024, 256)], sem_w.at[i, 1]),
                pltpu.make_async_copy(wv.at[rows], w_v.at[rows, pl.ds(1280, 256)], sem_w.at[i, 2]))

    def cache_copy(src, dst, sem, i):
        rows = pl.ds(pl.multiple_of(i * BCH, BCH), BCH)
        return pltpu.make_async_copy(src.at[rows], dst.at[rows], sem.at[i])

    def w_start(i):
        for cp in w_copies(i):
            cp.start()

    def cache_start(i):
        cache_copy(kc, k_v, sem_k, i).start()
        cache_copy(vc, v_v, sem_v, i).start()

    w_start(0)
    for cp in small:
        cp.wait()
    w_start(1)
    w_start(2)
    for r in range(0, ROWS, 16):
        x = x_v[r:r + 16, :].astype(F32)
        inv = lax.rsqrt(jnp.mean(x * x, axis=-1, keepdims=True) + 1e-5)
        n_v[r:r + 16, :] = (x * inv * gain_v[...].astype(F32).reshape(1, DIM)).astype(BF16)
    for b in range(ROWS):
        pos_v[b:b + 1, :] = jnp.full((1, HD), pos_s[b], jnp.int32)
    pair = lax.broadcasted_iota(jnp.int32, (8, HD), 1) // 2
    freq = jnp.full((8, HD), float(INV_FREQ[0]), F32)
    for i in range(1, HD // 2):
        freq = jnp.where(pair == i, float(INV_FREQ[i]), freq)
    angles = pos_v[...].astype(F32) * freq[0:1, :]
    cos_a = jnp.cos(angles)
    sin_a = jnp.sin(angles)
    odd = lax.broadcasted_iota(jnp.int32, (ROWS, HD), 1) % 2 == 1
    sin_a = jnp.where(odd, sin_a, -sin_a)

    after = {0: (3,), 1: (4, 5), 2: (6,), 3: (7,), 4: (8,)}
    for i in range(KCH):
        for cp in w_copies(i):
            cp.wait()
        for nxt in after[i]:
            if nxt < KCH:
                w_start(nxt)
            else:
                cache_start(nxt - KCH)
        rows = slice(i * KSTEP, (i + 1) * KSTEP)
        prod = jnp.dot(n_v[:, rows], w_v[rows, :], preferred_element_type=F32)
        acc[...] = prod if i == 0 else acc[...] + prod

    def rotate(val):
        swapped = jnp.where(odd, pltpu.roll(val, 1, 1), pltpu.roll(val, HD - 1, 1))
        return (val * cos_a + swapped * sin_a).astype(BF16).astype(F32)

    for h in range(HEADS):
        qs[pl.ds(h, ROWS, stride=HEADS), :] = rotate(acc[:, h * HD:(h + 1) * HD])
    for h in range(KV):
        lo = (HEADS + h) * HD
        ks[pl.ds(h, ROWS, stride=KV), :] = rotate(acc[:, lo:lo + HD])
        lo = (HEADS + KV + h) * HD
        vs[pl.ds(h, ROWS, stride=KV), :] = acc[:, lo:lo + HD].astype(BF16).astype(F32)
    kn_v[...] = ks[...].astype(BF16)
    vn_v[...] = vs[...].astype(BF16)
    new_copies = [pltpu.make_async_copy(kn_v, kn_ref, sem_n.at[0]), pltpu.make_async_copy(vn_v, vn_ref, sem_n.at[1])]
    for cp in new_copies:
        cp.start()

    row16 = lax.broadcasted_iota(jnp.int32, (16, HD), 0)
    lane = lax.broadcasted_iota(jnp.int32, (HEADS, KV * BLK), 1)
    group = lax.broadcasted_iota(jnp.int32, (HEADS, KV * BLK), 0) // (HEADS // KV)
    same_head = (lane % KV) == group
    lane_slot = lane // KV
    stat_lane = lax.broadcasted_iota(jnp.int32, (HEADS, HD), 1)

    def put_new(cache_v, new, b, slot):
        inside = jnp.logical_and(slot >= 0, slot < BLK)
        tile = jnp.where(inside, slot // 8, 0)
        local = jnp.where(inside, slot - tile * 8, -1)
        at = pl.ds(pl.multiple_of(tile * 16, 16), 16)
        old = cache_v[b, at, :].astype(F32)
        both = jnp.where(row16 % 2 == 0, new[pl.ds(2 * b, 1), :], new[pl.ds(2 * b + 1, 1), :])
        cache_v[b, at, :] = jnp.where(row16 // 2 == local, both, old).astype(BF16)

    for i in range(NB):
        cache_copy(kc, k_v, sem_k, i).wait()
        cache_copy(vc, v_v, sem_v, i).wait()
        slots = [pos_s[i * BCH + u] - sp * BLK for u in range(BCH)]
        for u in range(BCH):
            put_new(k_v, ks, i * BCH + u, slots[u])
            put_new(v_v, vs, i * BCH + u, slots[u])
        cache_copy(k_v, ko, sem_ko, i).start()
        cache_copy(v_v, vo, sem_vo, i).start()
        raw = []
        for u in range(BCH):
            b = i * BCH + u
            q = qs[b * HEADS:(b + 1) * HEADS, :].astype(BF16)
            raw.append(lax.dot_general(q, k_v[b], (((1,), (1,)), ((), ())), preferred_element_type=F32))
        stat = jnp.zeros((HEADS, HD), F32)
        for u in range(BCH):
            b = i * BCH + u
            valid = jnp.logical_and(same_head, lane_slot <= slots[u])
            score = jnp.where(valid, raw[u] * (HD ** -0.5), NEG)
            top = jnp.max(score, axis=-1, keepdims=True)
            prob = jnp.where(valid, jnp.exp(score - top), 0.0)
            total = jnp.sum(prob, axis=-1, keepdims=True)
            part_ref[i, u * HEADS:(u + 1) * HEADS, :] = jnp.dot(prob.astype(BF16), v_v[b], preferred_element_type=F32)
            stat = jnp.where(stat_lane == u, top, stat)
            stat = jnp.where(stat_lane == u + 64, total, stat)
        part_ref[i, QROWS:QROWS + HEADS, :] = stat
    for i in range(NB):
        cache_copy(k_v, ko, sem_ko, i).wait()
        cache_copy(v_v, vo, sem_vo, i).wait()
    for cp in new_copies:
        cp.wait()


def attend(new_pos, x, gain, wq, wk, wv, kc, vc):
    args = [pltpu.with_memory_space_constraint(a, pltpu.HBM) for a in (new_pos, x, gain, wq, wk, wv, kc, vc)]
    cache = jax.ShapeDtypeStruct(kc.shape, BF16)
    new = jax.ShapeDtypeStruct((ROWS * KV, HD), BF16)
    return pl.pallas_call(
        attend_kernel,
        out_shape=(cache, cache, new, new, jax.ShapeDtypeStruct((NB, QROWS + HEADS, HD), F32)),
        in_specs=[ANY] * 8,
        out_specs=(ANY,) * 4 + (VM,),
        scratch_shapes=[
            pltpu.SMEM((ROWS,), jnp.int32),
            pltpu.VMEM((ROWS, DIM), BF16),
            pltpu.VMEM((DIM,), BF16),
            pltpu.VMEM((DIM, QKV), BF16),
            pltpu.VMEM(kc.shape, BF16),
            pltpu.VMEM(vc.shape, BF16),
            pltpu.VMEM((ROWS, DIM), BF16),
            pltpu.VMEM((ROWS, QKV), F32),
            pltpu.VMEM((ROWS, HD), jnp.int32),
            pltpu.VMEM((ROWS * HEADS, HD), F32),
            pltpu.VMEM((ROWS * KV, HD), F32),
            pltpu.VMEM((ROWS * KV, HD), F32),
            pltpu.VMEM((ROWS * KV, HD), BF16),
            pltpu.VMEM((ROWS * KV, HD), BF16),
            pltpu.SemaphoreType.DMA((3,)),
            pltpu.SemaphoreType.DMA((KCH, 3)),
            pltpu.SemaphoreType.DMA((NB,)),
            pltpu.SemaphoreType.DMA((NB,)),
            pltpu.SemaphoreType.DMA((NB,)),
            pltpu.SemaphoreType.DMA((NB,)),
            pltpu.SemaphoreType.DMA((2,)),
        ],
        compiler_params=pltpu.CompilerParams(vmem_limit_bytes=ATTEND_VMEM),
        name="attend",
    )(*args)


TP = 4
COLS = DIM // 4
HID = 896
HCH = HID // 128
RB = ROWS // TP
SUMS = (1, 2, 3)
SPREAD = (1, 3, 2)
LAND = (1, 3, 2)
CHUNKS = ((0, 512), (512, 768))
NC = len(CHUNKS)


def mix_kernel(part_ref, x_hbm, gain_hbm, wo, wg, wu, wd, out_ref,
               xb_v, gain_v, wo_v, wgu_v, wd_v,
               pa, pb, pc, at_o, lhs_v, mm, rs_buf, hfull, n2, act, act_b, ofull,
               sem_l, sem_g, sem_d, cs, cr, rs_s, rs_r, az_s, az_r, ay_s, ay_r, ac_s, ac_r,
               my_s, my_r, mc_s, mc_r, zr, gu_v):
    dp = lax.axis_index('dp')
    z = lax.axis_index('tp')
    sp = lax.axis_index('sp')
    y = sp // 2
    c = sp % 2
    sp_y = (1 - y) * 2 + c
    sp_c = y * 2 + (1 - c)
    sp_yc = (1 - y) * 2 + (1 - c)
    dev_y = (dp, z, sp_y)
    dev_c = (dp, z, sp_c)
    dev_z = [None] + [(dp, lax.rem(z + d, TP), sp) for d in range(1, TP)]

    from_z = [z] + [lax.rem(z + TP - d, TP) for d in range(1, TP)]

    def col_at(s):
        return pl.ds(pl.multiple_of(s * COLS, 128), COLS)

    def chunk_at(s, j):
        return pl.ds(pl.multiple_of(s * COLS + CHUNKS[j][0], 128), CHUNKS[j][1])

    def row_at(zz):
        return pl.ds(pl.multiple_of(zz * RB, RB), RB)

    loads = [pltpu.make_async_copy(wo.at[:, col_at(sp)], wo_v, sem_l.at[0]),
             pltpu.make_async_copy(x_hbm.at[row_at(z), col_at(sp)], xb_v, sem_l.at[1]),
             pltpu.make_async_copy(gain_hbm, gain_v, sem_l.at[2])]
    for cp in loads:
        cp.start()

    def gu_copies(j):
        cols = pl.ds(pl.multiple_of(sp * HID + j * 128, 128), 128)
        return (pltpu.make_async_copy(wg.at[:, cols], wgu_v.at[j, :, pl.ds(0, 128)], sem_g.at[j, 0]),
                pltpu.make_async_copy(wu.at[:, cols], wgu_v.at[j, :, pl.ds(128, 128)], sem_g.at[j, 1]))

    order = [sp, sp_c, sp_y, sp_yc]
    d_copies = [pltpu.make_async_copy(wd.at[pl.ds(pl.multiple_of(s * HID, 128), HID), col_at(sp)],
                                      wd_v.at[i], sem_d.at[i]) for i, s in enumerate(order)]

    has_l, has_r = z > 0, z < TP - 1
    dev_l = (dp, jnp.maximum(z - 1, 0), sp)
    dev_r = (dp, jnp.minimum(z + 1, TP - 1), sp)

    def signal(sem, dev, cond=None):
        if cond is None:
            pl.semaphore_signal(sem, inc=1, device_id=dev, device_id_type=MESH)
        else:
            @pl.when(cond)
            def _():
                pl.semaphore_signal(sem, inc=1, device_id=dev, device_id_type=MESH)

    def wait_if(sem, cond):
        @pl.when(cond)
        def _():
            pl.semaphore_wait(sem, 1)

    barrier = pltpu.get_barrier_semaphore()
    signal(barrier, dev_y)
    signal(barrier, dev_c)
    signal(barrier, dev_l, has_l)
    signal(barrier, dev_r, has_r)
    pl.semaphore_wait(barrier, 2 + has_l.astype(jnp.int32) + has_r.astype(jnp.int32))
    inner = jnp.logical_and(has_l, has_r)
    signal(zr.at[0], dev_l, inner)
    signal(zr.at[1], dev_r, inner)

    sends = []

    def push(src, dst, ssem, rsem, dev):
        cp = pltpu.make_async_remote_copy(src_ref=src, dst_ref=dst, send_sem=ssem, recv_sem=rsem,
                                          device_id=dev, device_id_type=MESH)
        cp.start()
        sends.append(cp)
        return cp

    lane = lax.broadcasted_iota(jnp.int32, (HEADS, HD), 1)

    def weights(s1, s2):
        top = jnp.maximum(s1, s2)
        a1 = jnp.exp(s1 - top)
        a2 = jnp.exp(s2 - top)
        total = a1 * pltpu.roll(s1, 64, 1) + a2 * pltpu.roll(s2, 64, 1)
        return top, a1, a2, total

    half = pl.multiple_of(c * 256, 256)
    st = slice(QROWS, QROWS + HEADS)
    first = [push(part_ref.at[(1 - c) * 2 + k], pa.at[k], cs.at[0, k], cr.at[0, k], dev_c) for k in range(2)]
    second = []
    for k in range(2):
        first[k].wait_recv()
        mine = part_ref.at[c * 2 + k]
        top, a1, a2, total = weights(mine[st, :], pa[k, st, :])
        for i in range(BCH):
            r = slice(i * 8, i * 8 + 8)
            pb[k, r, :] = a1[:, i:i + 1] * mine[r, :] + a2[:, i:i + 1] * pa[k, r, :]
        pb[k, st, :] = jnp.where(lane < 64, top, pltpu.roll(total, 64, 1))
        second.append(push(pb.at[k], pc.at[k], cs.at[1, k], cr.at[1, k], dev_y))
    wait_if(zr.at[0], z + 2 < TP)
    wait_if(zr.at[1], z - 2 >= 0)
    signal(zr.at[2], dev_l, z == 1)
    signal(zr.at[3], dev_r, z == 2)
    third = []
    for k in range(2):
        second[k].wait_recv()
        top, a1, a2, total = weights(pb[k, st, :], pc[k, st, :])
        a1 = a1 / total
        a2 = a2 / total
        for i in range(BCH):
            r = slice(i * 8, i * 8 + 8)
            to = pl.ds(pl.multiple_of(half + k * QROWS + i * 8, 8), 8)
            at_o[to, :] = a1[:, i:i + 1] * pb[k, r, :] + a2[:, i:i + 1] * pc[k, r, :]
        piece = at_o.at[pl.ds(pl.multiple_of(half + k * QROWS, QROWS), QROWS)]
        third.append(push(piece, piece, cs.at[2, k], cr.at[2, k], dev_c))
    for cp in third:
        cp.wait_recv()
    for j in range(HCH):
        for cp in gu_copies(j):
            cp.start()
    for cp in d_copies:
        cp.start()
    wait_if(zr.at[2], z == 0)
    wait_if(zr.at[3], z == TP - 1)
    for h in range(HEADS):
        lhs_v[:, h * HD:(h + 1) * HD] = at_o[pl.ds(h, ROWS, stride=HEADS), :].astype(BF16)

    def scatter(stage, j):
        cols = pl.ds(*CHUNKS[j])
        for d in SUMS:
            zz = lax.rem(z + d, TP)
            push(mm.at[stage, row_at(zz), cols], rs_buf.at[stage, d - 1, :, cols],
                 rs_s.at[stage, j, d - 1], rs_r.at[stage, j, d - 1], dev_z[d])

    def gather(stage, base, full):
        def blk(s, d, j):
            return full.at[row_at(from_z[d]), chunk_at(s, j)]

        def wait_in(ref, sem):
            pltpu.make_async_copy(ref, ref, sem).wait()

        for j in range(NC):
            cols = pl.ds(*CHUNKS[j])
            val = base(cols) + mm[stage, row_at(z), cols]
            for d in range(1, TP):
                wait_in(rs_buf.at[stage, d - 1, :, cols], rs_r.at[stage, j, d - 1])
                val = val + rs_buf[stage, d - 1, :, cols]
            full[row_at(z), chunk_at(sp, j)] = val
            own = blk(sp, 0, j)
            for d in SPREAD:
                push(own, own, az_s.at[stage, j, d - 1], az_r.at[stage, j, d - 1], dev_z[d])
            push(own, own, ay_s.at[stage, j, 0], ay_r.at[stage, j, 0], dev_y)
            push(own, own, ac_s.at[stage, j, 0], ac_r.at[stage, j, 0], dev_c)
        for j in range(NC):
            for d in LAND:
                ref = blk(sp, d, j)
                wait_in(ref, az_r.at[stage, j, d - 1])
                push(ref, ref, ay_s.at[stage, j, d], ay_r.at[stage, j, d], dev_y)
                push(ref, ref, ac_s.at[stage, j, d], ac_r.at[stage, j, d], dev_c)
        for j in range(NC):
            for d in (0,) + LAND:
                ref = blk(sp_y, d, j)
                wait_in(ref, ay_r.at[stage, j, d])
                push(ref, ref, ac_s.at[stage, j, TP + d], ac_r.at[stage, j, TP + d], dev_c)
        for j in range(NC):
            for d in range(TP):
                wait_in(blk(sp_c, d, j), ac_r.at[stage, j, d])
                wait_in(blk(sp_yc, d, j), ac_r.at[stage, j, TP + d])

    for cp in loads:
        cp.wait()
    for j in range(NC):
        cols = pl.ds(*CHUNKS[j])
        mm[0, :, cols] = jnp.dot(lhs_v[...], wo_v[:, cols], preferred_element_type=F32)
        scatter(0, j)
    gather(0, lambda cols: xb_v[:, cols].astype(F32), hfull)

    for r in range(0, ROWS, 16):
        h = hfull[r:r + 16, :]
        inv = lax.rsqrt(jnp.mean(h * h, axis=-1, keepdims=True) + 1e-5)
        n2[r:r + 16, :] = (h * inv * gain_v[...].astype(F32).reshape(1, DIM)).astype(BF16)

    def act_copies(j):
        own = act.at[sp, j]
        return (pltpu.make_async_remote_copy(src_ref=own, dst_ref=own, send_sem=my_s.at[j], recv_sem=my_r.at[j],
                                             device_id=dev_y, device_id_type=MESH),
                pltpu.make_async_remote_copy(src_ref=own, dst_ref=own, send_sem=mc_s.at[0, j], recv_sem=mc_r.at[0, j],
                                             device_id=dev_c, device_id_type=MESH))

    def fwd_copy(j):
        ref = act.at[sp_y, j]
        return pltpu.make_async_remote_copy(src_ref=ref, dst_ref=ref, send_sem=mc_s.at[1, j], recv_sem=mc_r.at[1, j],
                                            device_id=dev_c, device_id_type=MESH)

    for j in range(HCH):
        for cp in gu_copies(j):
            cp.wait()

    def hidden_dot(j):
        gu_v[j % 2] = jnp.dot(n2[...], wgu_v[j], preferred_element_type=F32)

    def hidden_act(j):
        gate = gu_v[j % 2, :, :128]
        val = gate * jax.nn.sigmoid(gate) * gu_v[j % 2, :, 128:]
        act[sp, j] = val.astype(BF16).astype(F32)
        for cp in act_copies(j):
            cp.start()

    hidden_dot(0)
    for j in range(1, HCH):
        hidden_dot(j)
        hidden_act(j - 1)
    hidden_act(HCH - 1)

    def down(i, s):
        for j in range(HCH):
            act_b[:, j * 128:(j + 1) * 128] = act[s, j].astype(BF16)
        d_copies[i].wait()
        for k in range(0, COLS, 256):
            prod = jnp.dot(act_b[...], wd_v[i, :, k:k + 256], preferred_element_type=F32)
            if i == 0:
                mm[1, :, k:k + 256] = prod
            else:
                mm[1, :, k:k + 256] += prod
            if i == 3:
                for j in range(NC):
                    if CHUNKS[j][0] + CHUNKS[j][1] == k + 256:
                        scatter(1, j)

    down(0, sp)
    for j in range(HCH):
        act_copies(j)[1].wait_recv()
    down(1, sp_c)
    for j in range(HCH):
        act_copies(j)[0].wait_recv()
        fwd_copy(j).start()
    down(2, sp_y)
    for j in range(HCH):
        fwd_copy(j).wait_recv()
    down(3, sp_yc)

    own_h = hfull.at[row_at(z), col_at(sp)]
    gather(1, lambda cols: own_h[:, cols], ofull)
    out_ref[...] = ofull[...].astype(BF16)

    for cp in sends:
        cp.wait_send()
    for j in range(HCH):
        for cp in act_copies(j):
            cp.wait_send()
        fwd_copy(j).wait_send()


def mix(part, x, gain, wo, wg, wu, wd):
    dma = pltpu.SemaphoreType.DMA
    return pl.pallas_call(
        mix_kernel,
        out_shape=jax.ShapeDtypeStruct((ROWS, DIM), BF16),
        in_specs=[VM] + [ANY] * 6,
        out_specs=VM,
        scratch_shapes=[
            pltpu.VMEM((RB, COLS), BF16),
            pltpu.VMEM((DIM,), BF16),
            pltpu.VMEM((1024, COLS), BF16),
            pltpu.VMEM((HCH, DIM, 256), BF16),
            pltpu.VMEM((4, HID, COLS), BF16),
            pltpu.VMEM((2, QROWS + HEADS, HD), F32),
            pltpu.VMEM((2, QROWS + HEADS, HD), F32),
            pltpu.VMEM((2, QROWS + HEADS, HD), F32),
            pltpu.VMEM((ROWS * HEADS, HD), F32),
            pltpu.VMEM((ROWS, 1024), BF16),
            pltpu.VMEM((2, ROWS, COLS), F32),
            pltpu.VMEM((2, TP - 1, RB, COLS), F32),
            pltpu.VMEM((ROWS, DIM), F32),
            pltpu.VMEM((ROWS, DIM), BF16),
            pltpu.VMEM((4, HCH, ROWS, 128), F32),
            pltpu.VMEM((ROWS, HID), BF16),
            pltpu.VMEM((ROWS, DIM), F32),
            dma((3,)), dma((HCH, 2)), dma((4,)),
            dma((3, 2)), dma((3, 2)),
            dma((2, NC, 3)), dma((2, NC, 3)),
            dma((2, NC, 3)), dma((2, NC, 3)),
            dma((2, NC, TP)), dma((2, NC, TP)),
            dma((2, NC, 2 * TP)), dma((2, NC, 2 * TP)),
            dma((HCH,)), dma((HCH,)),
            dma((2, HCH)), dma((2, HCH)),
            pltpu.SemaphoreType.REGULAR((4,)),
            pltpu.VMEM((2, ROWS, 256), F32),
        ],
        compiler_params=pltpu.CompilerParams(vmem_limit_bytes=MIX_VMEM, collective_id=0, has_side_effects=True),
        name="mix",
    )(part, x, gain, wo, wg, wu, wd)


def solution(mesh):
    def local_step(layer_in, new_pos, k_blk, v_blk, attn_gain, w_query, w_key, w_value, w_out, mlp_gain, w_gate, w_up, w_down):
        flat = (ROWS, BLK * KV, HD)
        k_out, v_out, k_new, v_new, part = attend(
            new_pos, layer_in, attn_gain, w_query, w_key, w_value,
            k_blk.reshape(flat), v_blk.reshape(flat))
        layer_out = mix(part, layer_in, mlp_gain, w_out, w_gate, w_up, w_down)
        return (layer_out, k_out.reshape(k_blk.shape), v_out.reshape(v_blk.shape),
                k_new.reshape(ROWS, KV, HD), v_new.reshape(ROWS, KV, HD))

    cache_spec = P('dp', 'sp', 'tp', None)
    new_spec = P('dp', 'tp', None)
    in_specs = (P('dp', None), P('dp'), cache_spec, cache_spec, P(None), P(None, 'tp'), P(None, 'tp'), P(None, 'tp'), P('tp', None), P(None), P(None, 'tp'), P(None, 'tp'), P('tp', None))
    out_specs = (P('dp', None), cache_spec, cache_spec, new_spec, new_spec)
    return jax.shard_map(local_step, mesh=mesh, in_specs=in_specs, out_specs=out_specs, check_vma=False)
```

```python
import functools

import jax
import jax.numpy as jnp
import numpy as np
from jax import lax
from jax.experimental import pallas as pl
from jax.experimental.pallas import tpu as pltpu
from jax.sharding import PartitionSpec as P

ROPE_THETA = 1000000
MESH = pl.DeviceIdType.MESH
F32 = jnp.float32
BF16 = jnp.bfloat16
NEG = float(np.finfo(np.float32).min)
ATTEND_VMEM = 48 * 1024 * 1024
MIX_VMEM = 48 * 1024 * 1024
ANY = pl.BlockSpec(memory_space=pltpu.HBM)
VM = pl.BlockSpec(memory_space=pltpu.VMEM)

HALF_IDX = np.arange(64, dtype=np.float32)
INV_FREQ = np.float32(1.0) / (np.float32(ROPE_THETA) ** (np.float32(2.0) * HALF_IDX / np.float32(128)))

ROWS = 64
DIM = 5120
HD = 128
HEADS = 8
KV = 2
BLK = 128
QKV = (HEADS + 2 * KV) * HD
KSTEP = 1024
KCH = DIM // KSTEP
BCH = 16
NB = ROWS // BCH
QROWS = BCH * HEADS


def attend_kernel(pos_hbm, x_hbm, gain_hbm, wq, wk, wv, kc, vc,
                  ko, vo, kn_ref, vn_ref, part_ref,
                  pos_s, x_v, gain_v, w_v, k_v, v_v, n_v, acc, pos_v, qs, ks, vs, kn_v, vn_v,
                  sem_m, sem_w, sem_k, sem_v, sem_ko, sem_vo, sem_n):
    sp = lax.axis_index('sp')

    small = [pltpu.make_async_copy(pos_hbm, pos_s, sem_m.at[0]),
             pltpu.make_async_copy(x_hbm, x_v, sem_m.at[1]),
             pltpu.make_async_copy(gain_hbm, gain_v, sem_m.at[2])]
    for cp in small:
        cp.start()

    def w_copies(i):
        rows = pl.ds(pl.multiple_of(i * KSTEP, KSTEP), KSTEP)
        return (pltpu.make_async_copy(wq.at[rows], w_v.at[rows, pl.ds(0, 1024)], sem_w.at[i, 0]),
                pltpu.make_async_copy(wk.at[rows], w_v.at[rows, pl.ds(1024, 256)], sem_w.at[i, 1]),
                pltpu.make_async_copy(wv.at[rows], w_v.at[rows, pl.ds(1280, 256)], sem_w.at[i, 2]))

    def cache_copy(src, dst, sem, i):
        rows = pl.ds(pl.multiple_of(i * BCH, BCH), BCH)
        return pltpu.make_async_copy(src.at[rows], dst.at[rows], sem.at[i])

    def w_start(i):
        for cp in w_copies(i):
            cp.start()

    def cache_start(i):
        cache_copy(kc, k_v, sem_k, i).start()
        cache_copy(vc, v_v, sem_v, i).start()

    w_start(0)
    for cp in small:
        cp.wait()
    w_start(1)
    w_start(2)
    for r in range(0, ROWS, 16):
        x = x_v[r:r + 16, :].astype(F32)
        inv = lax.rsqrt(jnp.mean(x * x, axis=-1, keepdims=True) + 1e-5)
        n_v[r:r + 16, :] = (x * inv * gain_v[...].astype(F32).reshape(1, DIM)).astype(BF16)
    for b in range(ROWS):
        pos_v[b:b + 1, :] = jnp.full((1, HD), pos_s[b], jnp.int32)
    pair = lax.broadcasted_iota(jnp.int32, (8, HD), 1) // 2
    freq = jnp.full((8, HD), float(INV_FREQ[0]), F32)
    for i in range(1, HD // 2):
        freq = jnp.where(pair == i, float(INV_FREQ[i]), freq)
    angles = pos_v[...].astype(F32) * freq[0:1, :]
    cos_a = jnp.cos(angles)
    sin_a = jnp.sin(angles)
    odd = lax.broadcasted_iota(jnp.int32, (ROWS, HD), 1) % 2 == 1
    sin_a = jnp.where(odd, sin_a, -sin_a)

    after = {0: (3,), 1: (4,), 2: (5, 6), 3: (7, 8), 4: ()}
    for i in range(KCH):
        for cp in w_copies(i):
            cp.wait()
        for nxt in after[i]:
            if nxt < KCH:
                w_start(nxt)
            else:
                cache_start(nxt - KCH)
        rows = slice(i * KSTEP, (i + 1) * KSTEP)
        prod = jnp.dot(n_v[:, rows], w_v[rows, :], preferred_element_type=F32)
        acc[...] = prod if i == 0 else acc[...] + prod

    def rotate(val):
        swapped = jnp.where(odd, pltpu.roll(val, 1, 1), pltpu.roll(val, HD - 1, 1))
        return (val * cos_a + swapped * sin_a).astype(BF16).astype(F32)

    for h in range(HEADS):
        qs[pl.ds(h, ROWS, stride=HEADS), :] = rotate(acc[:, h * HD:(h + 1) * HD])
    for h in range(KV):
        lo = (HEADS + h) * HD
        ks[pl.ds(h, ROWS, stride=KV), :] = rotate(acc[:, lo:lo + HD])
        lo = (HEADS + KV + h) * HD
        vs[pl.ds(h, ROWS, stride=KV), :] = acc[:, lo:lo + HD].astype(BF16).astype(F32)
    kn_v[...] = ks[...].astype(BF16)
    vn_v[...] = vs[...].astype(BF16)
    new_copies = [pltpu.make_async_copy(kn_v, kn_ref, sem_n.at[0]), pltpu.make_async_copy(vn_v, vn_ref, sem_n.at[1])]
    for cp in new_copies:
        cp.start()

    row16 = lax.broadcasted_iota(jnp.int32, (16, HD), 0)
    lane = lax.broadcasted_iota(jnp.int32, (HEADS, KV * BLK), 1)
    group = lax.broadcasted_iota(jnp.int32, (HEADS, KV * BLK), 0) // (HEADS // KV)
    same_head = (lane % KV) == group
    lane_slot = lane // KV
    stat_lane = lax.broadcasted_iota(jnp.int32, (HEADS, HD), 1)

    def put_new(cache_v, new, b, slot):
        inside = jnp.logical_and(slot >= 0, slot < BLK)
        tile = jnp.where(inside, slot // 8, 0)
        local = jnp.where(inside, slot - tile * 8, -1)
        at = pl.ds(pl.multiple_of(tile * 16, 16), 16)
        old = cache_v[b, at, :].astype(F32)
        both = jnp.where(row16 % 2 == 0, new[pl.ds(2 * b, 1), :], new[pl.ds(2 * b + 1, 1), :])
        cache_v[b, at, :] = jnp.where(row16 // 2 == local, both, old).astype(BF16)

    for i in range(NB):
        cache_copy(kc, k_v, sem_k, i).wait()
        cache_copy(vc, v_v, sem_v, i).wait()
        slots = [pos_s[i * BCH + u] - sp * BLK for u in range(BCH)]
        for u in range(BCH):
            put_new(k_v, ks, i * BCH + u, slots[u])
            put_new(v_v, vs, i * BCH + u, slots[u])
        cache_copy(k_v, ko, sem_ko, i).start()
        cache_copy(v_v, vo, sem_vo, i).start()
        raw = []
        for u in range(BCH):
            b = i * BCH + u
            q = qs[b * HEADS:(b + 1) * HEADS, :].astype(BF16)
            raw.append(lax.dot_general(q, k_v[b], (((1,), (1,)), ((), ())), preferred_element_type=F32))
        stat = jnp.zeros((HEADS, HD), F32)
        for u in range(BCH):
            b = i * BCH + u
            valid = jnp.logical_and(same_head, lane_slot <= slots[u])
            score = jnp.where(valid, raw[u] * (HD ** -0.5), NEG)
            top = jnp.max(score, axis=-1, keepdims=True)
            prob = jnp.where(valid, jnp.exp(score - top), 0.0)
            total = jnp.sum(prob, axis=-1, keepdims=True)
            part_ref[i, u * HEADS:(u + 1) * HEADS, :] = jnp.dot(prob.astype(BF16), v_v[b], preferred_element_type=F32)
            stat = jnp.where(stat_lane == u, top, stat)
            stat = jnp.where(stat_lane == u + 64, total, stat)
        part_ref[i, QROWS:QROWS + HEADS, :] = stat
    for i in range(NB):
        cache_copy(k_v, ko, sem_ko, i).wait()
        cache_copy(v_v, vo, sem_vo, i).wait()
    for cp in new_copies:
        cp.wait()


def attend(new_pos, x, gain, wq, wk, wv, kc, vc):
    args = [pltpu.with_memory_space_constraint(a, pltpu.HBM) for a in (new_pos, x, gain, wq, wk, wv, kc, vc)]
    cache = jax.ShapeDtypeStruct(kc.shape, BF16)
    new = jax.ShapeDtypeStruct((ROWS * KV, HD), BF16)
    return pl.pallas_call(
        attend_kernel,
        out_shape=(cache, cache, new, new, jax.ShapeDtypeStruct((NB, QROWS + HEADS, HD), F32)),
        in_specs=[ANY] * 8,
        out_specs=(ANY,) * 4 + (VM,),
        scratch_shapes=[
            pltpu.SMEM((ROWS,), jnp.int32),
            pltpu.VMEM((ROWS, DIM), BF16),
            pltpu.VMEM((DIM,), BF16),
            pltpu.VMEM((DIM, QKV), BF16),
            pltpu.VMEM(kc.shape, BF16),
            pltpu.VMEM(vc.shape, BF16),
            pltpu.VMEM((ROWS, DIM), BF16),
            pltpu.VMEM((ROWS, QKV), F32),
            pltpu.VMEM((ROWS, HD), jnp.int32),
            pltpu.VMEM((ROWS * HEADS, HD), F32),
            pltpu.VMEM((ROWS * KV, HD), F32),
            pltpu.VMEM((ROWS * KV, HD), F32),
            pltpu.VMEM((ROWS * KV, HD), BF16),
            pltpu.VMEM((ROWS * KV, HD), BF16),
            pltpu.SemaphoreType.DMA((3,)),
            pltpu.SemaphoreType.DMA((KCH, 3)),
            pltpu.SemaphoreType.DMA((NB,)),
            pltpu.SemaphoreType.DMA((NB,)),
            pltpu.SemaphoreType.DMA((NB,)),
            pltpu.SemaphoreType.DMA((NB,)),
            pltpu.SemaphoreType.DMA((2,)),
        ],
        compiler_params=pltpu.CompilerParams(vmem_limit_bytes=ATTEND_VMEM),
        name="attend",
    )(*args)


TP = 4
COLS = DIM // 4
HID = 896
HCH = HID // 128
EXTRA = 3
SENT = HCH - EXTRA
RB = ROWS // TP
SUMS = (1, 2, 3)
SPREAD = (1, 3, 2)
LAND = (1, 3, 2)
RELAYED = (0, 1)
NEAREST = (0, 1)
CHUNKS = ((0, 512), (512, 256), (768, 512))
NC = len(CHUNKS)


def mix_kernel(part_ref, x_hbm, gain_hbm, wo, wg, wu, wd, out_ref,
               xb_v, gain_v, wo_v, wgu_v, wd_v,
               pa, pb, pc, at_o, lhs_v, mm, rs_buf, hfull, n2, act, act_b, ofull,
               sem_l, sem_g, sem_d, cs, cr, rs_s, rs_r, az_s, az_r, ay_s, ay_r, ac_s, ac_r,
               my_s, my_r, mc_s, mc_r, zr, gu_v, zf_s):
    dp = lax.axis_index('dp')
    z = lax.axis_index('tp')
    sp = lax.axis_index('sp')
    y = sp // 2
    c = sp % 2
    sp_y = (1 - y) * 2 + c
    sp_c = y * 2 + (1 - c)
    sp_yc = (1 - y) * 2 + (1 - c)
    dev_y = (dp, z, sp_y)
    dev_c = (dp, z, sp_c)
    dev_z = [None] + [(dp, lax.rem(z + d, TP), sp) for d in range(1, TP)]

    from_z = [z] + [lax.rem(z + TP - d, TP) for d in range(1, TP)]

    def col_at(s):
        return pl.ds(pl.multiple_of(s * COLS, 128), COLS)

    def chunk_at(s, j):
        return pl.ds(pl.multiple_of(s * COLS + CHUNKS[j][0], 128), CHUNKS[j][1])

    def row_at(zz):
        return pl.ds(pl.multiple_of(zz * RB, RB), RB)

    loads = [pltpu.make_async_copy(wo.at[:, col_at(sp)], wo_v, sem_l.at[0]),
             pltpu.make_async_copy(x_hbm.at[row_at(z), col_at(sp)], xb_v, sem_l.at[1]),
             pltpu.make_async_copy(gain_hbm, gain_v, sem_l.at[2])]
    for cp in loads:
        cp.start()

    def gu_copies(j):
        at = sp * HID + j * 128 if j < HCH else sp_y * HID + (j - EXTRA) * 128
        cols = pl.ds(pl.multiple_of(at, 128), 128)
        return (pltpu.make_async_copy(wg.at[:, cols], wgu_v.at[j, :, pl.ds(0, 128)], sem_g.at[j, 0]),
                pltpu.make_async_copy(wu.at[:, cols], wgu_v.at[j, :, pl.ds(128, 128)], sem_g.at[j, 1]))

    order = [sp, sp_c, sp_y, sp_yc]
    d_copies = [pltpu.make_async_copy(wd.at[pl.ds(pl.multiple_of(s * HID, 128), HID), col_at(sp)],
                                      wd_v.at[i], sem_d.at[i]) for i, s in enumerate(order)]

    has_l, has_r = z > 0, z < TP - 1
    dev_l = (dp, jnp.maximum(z - 1, 0), sp)
    dev_r = (dp, jnp.minimum(z + 1, TP - 1), sp)

    def signal(sem, dev, cond=None):
        if cond is None:
            pl.semaphore_signal(sem, inc=1, device_id=dev, device_id_type=MESH)
        else:
            @pl.when(cond)
            def _():
                pl.semaphore_signal(sem, inc=1, device_id=dev, device_id_type=MESH)

    def wait_if(sem, cond):
        @pl.when(cond)
        def _():
            pl.semaphore_wait(sem, 1)

    barrier = pltpu.get_barrier_semaphore()
    signal(barrier, dev_y)
    signal(barrier, dev_c)
    signal(barrier, dev_l, has_l)
    signal(barrier, dev_r, has_r)
    pl.semaphore_wait(barrier, 2 + has_l.astype(jnp.int32) + has_r.astype(jnp.int32))
    inner = jnp.logical_and(has_l, has_r)
    signal(zr.at[0], dev_l, inner)
    signal(zr.at[1], dev_r, inner)

    sends = []

    def push(src, dst, ssem, rsem, dev):
        cp = pltpu.make_async_remote_copy(src_ref=src, dst_ref=dst, send_sem=ssem, recv_sem=rsem,
                                          device_id=dev, device_id_type=MESH)
        cp.start()
        sends.append(cp)
        return cp

    lane = lax.broadcasted_iota(jnp.int32, (HEADS, HD), 1)

    def weights(s1, s2):
        top = jnp.maximum(s1, s2)
        a1 = jnp.exp(s1 - top)
        a2 = jnp.exp(s2 - top)
        total = a1 * pltpu.roll(s1, 64, 1) + a2 * pltpu.roll(s2, 64, 1)
        return top, a1, a2, total

    half = pl.multiple_of(c * 256, 256)
    st = slice(QROWS, QROWS + HEADS)
    first = [push(part_ref.at[(1 - c) * 2 + k], pa.at[k], cs.at[0, k], cr.at[0, k], dev_c) for k in range(2)]
    second = []
    for k in range(2):
        first[k].wait_recv()
        mine = part_ref.at[c * 2 + k]
        top, a1, a2, total = weights(mine[st, :], pa[k, st, :])
        for i in range(BCH):
            r = slice(i * 8, i * 8 + 8)
            pb[k, r, :] = a1[:, i:i + 1] * mine[r, :] + a2[:, i:i + 1] * pa[k, r, :]
        pb[k, st, :] = jnp.where(lane < 64, top, pltpu.roll(total, 64, 1))
        second.append(push(pb.at[k], pc.at[k], cs.at[1, k], cr.at[1, k], dev_y))
    wait_if(zr.at[0], z + 2 < TP)
    wait_if(zr.at[1], z - 2 >= 0)
    signal(zr.at[2], dev_l, z == 1)
    signal(zr.at[3], dev_r, z == 2)
    third = []
    for k in range(2):
        second[k].wait_recv()
        top, a1, a2, total = weights(pb[k, st, :], pc[k, st, :])
        a1 = a1 / total
        a2 = a2 / total
        for i in range(BCH):
            r = slice(i * 8, i * 8 + 8)
            to = pl.ds(pl.multiple_of(half + k * QROWS + i * 8, 8), 8)
            at_o[to, :] = a1[:, i:i + 1] * pb[k, r, :] + a2[:, i:i + 1] * pc[k, r, :]
        piece = at_o.at[pl.ds(pl.multiple_of(half + k * QROWS, QROWS), QROWS)]
        third.append(push(piece, piece, cs.at[2, k], cr.at[2, k], dev_c))
    for cp in third:
        cp.wait_recv()
    for j in range(HCH + EXTRA):
        for cp in gu_copies(j):
            cp.start()
    for cp in d_copies:
        cp.start()
    wait_if(zr.at[2], z == 0)
    wait_if(zr.at[3], z == TP - 1)
    for h in range(HEADS):
        lhs_v[:, h * HD:(h + 1) * HD] = at_o[pl.ds(h, ROWS, stride=HEADS), :].astype(BF16)

    def scatter(stage, j):
        cols = pl.ds(*CHUNKS[j])
        for d in SUMS:
            zz = lax.rem(z + d, TP)
            push(mm.at[stage, row_at(zz), cols], rs_buf.at[stage, d - 1, :, cols],
                 rs_s.at[stage, j, d - 1], rs_r.at[stage, j, d - 1], dev_z[d])

    mate = z + 1 - 2 * lax.rem(z, 2)
    cross = jnp.where(z < 2, 2, 1)
    near = [z, jnp.where(z < 2, z + 1, z - 1),
            jnp.where(z == 0, 2, jnp.where(z == TP - 1, 1, mate)),
            jnp.where(z < 2, TP - 1, 0)]

    def source(j, k):
        return near[k] if j in NEAREST else from_z[((0,) + LAND)[k]]

    def relay(stage, j, src, start):
        full = ofull if stage else hfull
        ref = full.at[row_at(src), chunk_at(sp, j)]

        @pl.when(jnp.logical_and(inner, src // 2 != z // 2))
        def _():
            to = lax.rem(mate - src + TP, TP) - 1
            cp = pltpu.make_async_remote_copy(src_ref=ref, dst_ref=ref,
                                              send_sem=zf_s.at[stage, j, lax.rem(z - src + TP, TP) - 1],
                                              recv_sem=az_r.at[stage, j, to], device_id=(dp, mate, sp),
                                              device_id_type=MESH)
            if start:
                cp.start()
            else:
                cp.wait_send()

    def gather(stage, base, full):
        def blk(s, k, j):
            return full.at[row_at(source(j, k)), chunk_at(s, j)]

        def wait_in(ref, sem):
            pltpu.make_async_copy(ref, ref, sem).wait()

        for j in range(NC):
            cols = pl.ds(*CHUNKS[j])
            val = base(cols) + mm[stage, row_at(z), cols]
            for d in range(1, TP):
                wait_in(rs_buf.at[stage, d - 1, :, cols], rs_r.at[stage, j, d - 1])
                val = val + rs_buf[stage, d - 1, :, cols]
            full[row_at(z), chunk_at(sp, j)] = val
            own = blk(sp, 0, j)
            if j in RELAYED:
                push(own, own, az_s.at[stage, j, 0], az_r.at[stage, j, lax.rem(cross - z + TP, TP) - 1], (dp, cross, sp))
                push(own, own, az_s.at[stage, j, 1], az_r.at[stage, j, lax.rem(mate - z + TP, TP) - 1], (dp, mate, sp))
            else:
                for d in SPREAD:
                    push(own, own, az_s.at[stage, j, d - 1], az_r.at[stage, j, d - 1], dev_z[d])
            push(own, own, ay_s.at[stage, j, 0], ay_r.at[stage, j, 0], dev_y)
            push(own, own, ac_s.at[stage, j, 0], ac_r.at[stage, j, 0], dev_c)
        for j in range(NC):
            for d in range(1, TP):
                ref = blk(sp, d, j)
                wait_in(ref, az_r.at[stage, j, lax.rem(z - source(j, d) + TP, TP) - 1])
                if j in RELAYED:
                    relay(stage, j, source(j, d), True)
                push(ref, ref, ay_s.at[stage, j, d], ay_r.at[stage, j, d], dev_y)
                push(ref, ref, ac_s.at[stage, j, d], ac_r.at[stage, j, d], dev_c)
        for j in range(NC):
            for d in range(TP):
                ref = blk(sp_y, d, j)
                wait_in(ref, ay_r.at[stage, j, d])
                push(ref, ref, ac_s.at[stage, j, TP + d], ac_r.at[stage, j, TP + d], dev_c)
        for j in range(NC):
            for d in range(TP):
                wait_in(blk(sp_c, d, j), ac_r.at[stage, j, d])
                wait_in(blk(sp_yc, d, j), ac_r.at[stage, j, TP + d])

    for cp in loads:
        cp.wait()
    for j in range(NC):
        cols = pl.ds(*CHUNKS[j])
        mm[0, :, cols] = jnp.dot(lhs_v[...], wo_v[:, cols], preferred_element_type=F32)
        scatter(0, j)
    gather(0, lambda cols: xb_v[:, cols].astype(F32), hfull)

    for r in range(0, ROWS, 16):
        h = hfull[r:r + 16, :]
        inv = lax.rsqrt(jnp.mean(h * h, axis=-1, keepdims=True) + 1e-5)
        n2[r:r + 16, :] = (h * inv * gain_v[...].astype(F32).reshape(1, DIM)).astype(BF16)

    def act_copies(j):
        own = act.at[sp, j]
        return (pltpu.make_async_remote_copy(src_ref=own, dst_ref=own, send_sem=my_s.at[j], recv_sem=my_r.at[j],
                                             device_id=dev_y, device_id_type=MESH),
                pltpu.make_async_remote_copy(src_ref=own, dst_ref=own, send_sem=mc_s.at[0, j], recv_sem=mc_r.at[0, j],
                                             device_id=dev_c, device_id_type=MESH))

    def fwd_copy(j):
        ref = act.at[sp_y, j]
        return pltpu.make_async_remote_copy(src_ref=ref, dst_ref=ref, send_sem=mc_s.at[1, j], recv_sem=mc_r.at[1, j],
                                            device_id=dev_c, device_id_type=MESH)

    for j in range(HCH + EXTRA):
        for cp in gu_copies(j):
            cp.wait()

    def hidden_dot(j):
        gu_v[j % 2] = jnp.dot(n2[...], wgu_v[j], preferred_element_type=F32)

    def hidden_act(j):
        gate = gu_v[j % 2, :, :128]
        val = (gate * jax.nn.sigmoid(gate) * gu_v[j % 2, :, 128:]).astype(BF16).astype(F32)
        if j < HCH:
            act[sp, j] = val
            to_y, to_c = act_copies(j)
            if j < SENT:
                to_y.start()
            to_c.start()
        else:
            act[sp_y, j - EXTRA] = val
            fwd_copy(j - EXTRA).start()

    hidden_dot(0)
    for j in range(1, HCH + EXTRA):
        hidden_dot(j)
        hidden_act(j - 1)
    hidden_act(HCH + EXTRA - 1)

    def down(i, s):
        for j in range(HCH):
            act_b[:, j * 128:(j + 1) * 128] = act[s, j].astype(BF16)
        d_copies[i].wait()
        for k in range(0, COLS, 256):
            prod = jnp.dot(act_b[...], wd_v[i, :, k:k + 256], preferred_element_type=F32)
            if i == 0:
                mm[1, :, k:k + 256] = prod
            else:
                mm[1, :, k:k + 256] += prod
            if i == 3:
                for j in range(NC):
                    if CHUNKS[j][0] + CHUNKS[j][1] == k + 256:
                        scatter(1, j)

    down(0, sp)
    for j in range(HCH):
        act_copies(j)[1].wait_recv()
    down(1, sp_c)
    for j in range(SENT):
        act_copies(j)[0].wait_recv()
        fwd_copy(j).start()
    down(2, sp_y)
    for j in range(HCH):
        fwd_copy(j).wait_recv()
    down(3, sp_yc)

    own_h = hfull.at[row_at(z), col_at(sp)]
    gather(1, lambda cols: own_h[:, cols], ofull)
    out_ref[...] = ofull[...].astype(BF16)

    for cp in sends:
        cp.wait_send()
    for stage in range(2):
        for j in RELAYED:
            for d in range(1, TP):
                relay(stage, j, source(j, d), False)
    for j in range(HCH):
        to_y, to_c = act_copies(j)
        if j < SENT:
            to_y.wait_send()
        to_c.wait_send()
        fwd_copy(j).wait_send()


def mix(part, x, gain, wo, wg, wu, wd):
    dma = pltpu.SemaphoreType.DMA
    return pl.pallas_call(
        mix_kernel,
        out_shape=jax.ShapeDtypeStruct((ROWS, DIM), BF16),
        in_specs=[VM] + [ANY] * 6,
        out_specs=VM,
        scratch_shapes=[
            pltpu.VMEM((RB, COLS), BF16),
            pltpu.VMEM((DIM,), BF16),
            pltpu.VMEM((1024, COLS), BF16),
            pltpu.VMEM((HCH + EXTRA, DIM, 256), BF16),
            pltpu.VMEM((4, HID, COLS), BF16),
            pltpu.VMEM((2, QROWS + HEADS, HD), F32),
            pltpu.VMEM((2, QROWS + HEADS, HD), F32),
            pltpu.VMEM((2, QROWS + HEADS, HD), F32),
            pltpu.VMEM((ROWS * HEADS, HD), F32),
            pltpu.VMEM((ROWS, 1024), BF16),
            pltpu.VMEM((2, ROWS, COLS), F32),
            pltpu.VMEM((2, TP - 1, RB, COLS), F32),
            pltpu.VMEM((ROWS, DIM), F32),
            pltpu.VMEM((ROWS, DIM), BF16),
            pltpu.VMEM((4, HCH, ROWS, 128), F32),
            pltpu.VMEM((ROWS, HID), BF16),
            pltpu.VMEM((ROWS, DIM), F32),
            dma((3,)), dma((HCH + EXTRA, 2)), dma((4,)),
            dma((3, 2)), dma((3, 2)),
            dma((2, NC, 3)), dma((2, NC, 3)),
            dma((2, NC, 3)), dma((2, NC, 3)),
            dma((2, NC, TP)), dma((2, NC, TP)),
            dma((2, NC, 2 * TP)), dma((2, NC, 2 * TP)),
            dma((HCH,)), dma((HCH,)),
            dma((2, HCH)), dma((2, HCH)),
            pltpu.SemaphoreType.REGULAR((4,)),
            pltpu.VMEM((2, ROWS, 256), F32),
            dma((2, NC, 3)),
        ],
        compiler_params=pltpu.CompilerParams(vmem_limit_bytes=MIX_VMEM, collective_id=0, has_side_effects=True),
        name="mix",
    )(part, x, gain, wo, wg, wu, wd)


def solution(mesh):
    def local_step(layer_in, new_pos, k_blk, v_blk, attn_gain, w_query, w_key, w_value, w_out, mlp_gain, w_gate, w_up, w_down):
        flat = (ROWS, BLK * KV, HD)
        k_out, v_out, k_new, v_new, part = attend(
            new_pos, layer_in, attn_gain, w_query, w_key, w_value,
            k_blk.reshape(flat), v_blk.reshape(flat))
        layer_out = mix(part, layer_in, mlp_gain, w_out, w_gate, w_up, w_down)
        return (layer_out, k_out.reshape(k_blk.shape), v_out.reshape(v_blk.shape),
                k_new.reshape(ROWS, KV, HD), v_new.reshape(ROWS, KV, HD))

    cache_spec = P('dp', 'sp', 'tp', None)
    new_spec = P('dp', 'tp', None)
    in_specs = (P('dp', None), P('dp'), cache_spec, cache_spec, P(None), P(None, 'tp'), P(None, 'tp'), P(None, 'tp'), P('tp', None), P(None), P(None, 'tp'), P(None, 'tp'), P('tp', None))
    out_specs = (P('dp', None), cache_spec, cache_spec, new_spec, new_spec)
    return jax.shard_map(local_step, mesh=mesh, in_specs=in_specs, out_specs=out_specs, check_vma=False)
```
